8 devices in a mesh: col: 4 (over z, y, x), row: 2 (over core).
Axes of the slice: x: 2, y: 2, z: 1, core: 2. Of those that a mesh axis runs over, the one named last changes fastest.
Arguments:
- inter_mask: int32 [32768, 4096], P('row', 'col')
- emb_user: bfloat16 [32768, 64], P(('row', 'col'))
- emb_item: bfloat16 [4096, 64], P(('col', 'row'))
- triples: int32 [128, 3], replicated
Outputs:
- output 1: bfloat16 [32768, 64], P(('row', 'col'))
- output 2: bfloat16 [4096, 64], P(('col', 'row'))
- output 3: float32 [], replicated
All inputs are finite; a program needn't handle non-finite values.
Results may differ from the reference program's by a relative error of at most 0.00529452.
Values are sent between devices in bfloat16 or wider.
A program may use at most 1 GiB of HBM per device.

```python
import jax
import jax.numpy as jnp
from jax import lax

USERS = 32768
ITEMS = 4096
DIM = 64
LAYERS = 3
TRIPLES = 128
USER_DEGREE = 3


def draw_triples(trip_key):
    key_user, key_pos, key_neg = jax.random.split(trip_key, 3)
    row_pos = jnp.arange(TRIPLES)
    user_ids = jax.random.randint(key_user, (TRIPLES,), 0, USERS)
    pos_ids = jax.random.randint(key_pos, (TRIPLES,), 0, ITEMS)
    neg_ids = jax.random.randint(key_neg, (TRIPLES,), 0, ITEMS)
    user_ids = jnp.where(row_pos == 0, USERS - 1, jnp.where(row_pos == 1, 0, user_ids))
    pos_ids = jnp.where(row_pos == 0, ITEMS - 1, jnp.where(row_pos == 1, 0, pos_ids))
    neg_ids = jnp.where(row_pos == 0, 0, jnp.where(row_pos == 1, ITEMS - 1, neg_ids))
    return jnp.stack([user_ids, pos_ids, neg_ids], axis=1).astype(jnp.int32)


def setup_inputs(seed: int = 0) -> dict:
    base_key = jax.random.key(seed)
    key_mask, key_user, key_item, key_trip = jax.random.split(base_key, 4)
    raw_draw = jax.random.randint(key_mask, (USERS, ITEMS), 0, ITEMS)
    inter_mask = (raw_draw < USER_DEGREE).astype(jnp.int32)
    emb_user = jax.random.normal(key_user, (USERS, DIM), jnp.float32).astype(jnp.bfloat16)
    emb_item = jax.random.normal(key_item, (ITEMS, DIM), jnp.float32).astype(jnp.bfloat16)
    return {"inter_mask": inter_mask, "emb_user": emb_user, "emb_item": emb_item, "triples": draw_triples(key_trip)}


def reference(inter_mask, emb_user, emb_item, triples):
    deg_user = jnp.maximum(jnp.sum(inter_mask, axis=1), 1)
    deg_item = jnp.maximum(jnp.sum(inter_mask, axis=0), 1)
    scale_user = lax.rsqrt(deg_user.astype(jnp.float32))
    scale_item = lax.rsqrt(deg_item.astype(jnp.float32))
    norm_adj = (inter_mask.astype(jnp.float32) * scale_user[:, None] * scale_item[None, :]).astype(jnp.bfloat16)
    layer_user = emb_user
    layer_item = emb_item
    total_user = emb_user.astype(jnp.float32)
    total_item = emb_item.astype(jnp.float32)
    for layer_idx in range(LAYERS):
        next_user = jnp.dot(norm_adj, layer_item, preferred_element_type=jnp.float32).astype(jnp.bfloat16)
        next_item = lax.dot_general(norm_adj, layer_user, (((0,), (0,)), ((), ())), preferred_element_type=jnp.float32).astype(jnp.bfloat16)
        total_user = total_user + next_user.astype(jnp.float32)
        total_item = total_item + next_item.astype(jnp.float32)
        layer_user = next_user
        layer_item = next_item
    out_user = (total_user / (LAYERS + 1)).astype(jnp.bfloat16)
    out_item = (total_item / (LAYERS + 1)).astype(jnp.bfloat16)
    user_vec = jnp.take(out_user, triples[:, 0], axis=0).astype(jnp.float32)
    pos_vec = jnp.take(out_item, triples[:, 1], axis=0).astype(jnp.float32)
    neg_vec = jnp.take(out_item, triples[:, 2], axis=0).astype(jnp.float32)
    margin = jnp.sum(user_vec * pos_vec, axis=1) - jnp.sum(user_vec * neg_vec, axis=1)
    bpr_loss = jnp.mean(jax.nn.softplus(-margin))
    return out_user, out_item, bpr_loss
```

```python
import functools

import jax
import jax.numpy as jnp
from jax import lax
from jax.experimental import pallas as pl
from jax.experimental.pallas import tpu as pltpu
from jax.sharding import PartitionSpec as P

LAYERS = 3
NC = 4
MESH = pl.DeviceIdType.MESH
F32 = jnp.float32
BF16 = jnp.bfloat16
NT = (((1,), (1,)), ((), ()))


def flip(v, f):
    return v + f - 2 * v * f


def kernel(mask, emb_user, emb_item, triples, out_user, out_item, loss,
           adj, ring, part, recv1, recv2, table, acc, racc, items, eu_in, ei_in, ei_half,
           rowsum, deg, rdeg, col, rcol, su, sv, ubuf, ibuf, picks, rpicks, lbuf,
           ring_sem, in_sem, out_sem, item_sem, deg_s, deg_r, col_sem,
           ag0_s, ag0_r, fw0_s, fw0_r, s1, r1, s2, r2, ag_s, ag_r, fw_s, fw_r, acc_s, acc_r,
           pick_s, pick_r, loss_s, loss_r):
    dim = emb_user.shape[1]
    users, nitem = mask.shape
    shard = users // 4
    half = shard // 2
    width = half // NC
    nhalf = nitem // 2
    c = lax.axis_index("col")
    r = lax.axis_index("row")
    x = c % 2
    y = c // 2
    nx = y * 2 + 1 - x
    ny = (1 - y) * 2 + x
    nd = (1 - y) * 2 + 1 - x

    def dev(col_id):
        return {"col": col_id, "row": r}

    partner = {"col": c, "row": 1 - r}

    def remote(src, dst, ss, rs, device):
        return pltpu.make_async_remote_copy(src_ref=src, dst_ref=dst, send_sem=ss, recv_sem=rs,
                                            device_id=device, device_id_type=MESH)

    blk = ring.shape[1]
    nslot = ring.shape[0]
    nblk = users // blk

    def mask_copy(b, slot):
        return pltpu.make_async_copy(mask.at[pl.ds(b * blk, blk)], ring.at[slot], ring_sem.at[slot])

    cu = pltpu.make_async_copy(emb_user, eu_in, in_sem.at[0])
    ci = pltpu.make_async_copy(emb_item, ei_in, in_sem.at[1])
    cu.start()
    ci.start()
    for b in range(nslot):
        mask_copy(b, b).start()

    barrier = pltpu.get_barrier_semaphore()
    for dc in (c, nx, ny, nd):
        for dr in (r, 1 - r):
            if dc is c and dr is r:
                continue
            pl.semaphore_signal(barrier, inc=1, device_id={"col": dc, "row": dr}, device_id_type=MESH)
    pl.semaphore_wait(barrier, 7)

    cu.wait()
    ci.wait()

    def tr_user(n, carry):
        hh = n // NC
        kk = n % NC
        rows = eu_in[pl.ds(pl.multiple_of(n * width, width), width), :]
        table[0, 0, hh, kk] = rows.astype(F32).T.astype(BF16)
        return carry

    lax.fori_loop(0, 2 * NC, tr_user, 0)
    ei_half[r] = ei_in[...].astype(F32).T.astype(BF16)
    ic = remote(ei_half.at[r], ei_half.at[r], item_sem.at[0], item_sem.at[1], partner)
    ic.start()

    def ag0(d, hh):
        return remote(table.at[0, 0, hh], table.at[0, 1 + d, hh], ag0_s.at[d, hh], ag0_r.at[d, hh],
                      dev(nx if d == 0 else ny))

    def fw0(hh):
        return remote(table.at[0, 1 + hh, hh], table.at[0, 3, hh], fw0_s.at[hh], fw0_r.at[hh],
                      dev(ny if hh == 0 else nx))

    for d, hh in ((0, 0), (1, 1), (0, 1), (1, 0)):
        ag0(d, hh).start()

    strip = 32
    col[...] = jnp.zeros_like(col)
    ones = jnp.ones((16, 128), BF16)
    sub8 = lax.broadcasted_iota(jnp.int32, (8, 128), 0)
    pair = 2 * blk
    groups = pair // 128

    def read_pair(i):
        for u in range(2):
            slot = (i % 2) * 2 + u
            b = i * 2 + u
            mask_copy(b, slot).wait()

            def strips(q, colacc):
                r0 = pl.multiple_of(q * strip, strip)
                m = ring[slot, pl.ds(r0, strip), :]
                mb = m.astype(F32).astype(BF16)
                adj[pl.ds(pl.multiple_of(b * blk + q * strip, strip), strip), :] = mb
                rsum = mb[:, 0:128]
                for j in range(1, nitem // 128):
                    rsum = rsum + mb[:, j * 128:(j + 1) * 128]
                rowsum[pl.ds(pl.multiple_of(u * blk + q * strip, strip), strip), :] = rsum
                for j in range(strip // 8):
                    colacc = colacc + m[j * 8:(j + 1) * 8, :]
                return colacc

            colacc = lax.fori_loop(0, blk // strip, strips, jnp.zeros((8, nitem), jnp.int32))
            col[...] += colacc.astype(F32)

            @pl.when(b + nslot < nblk)
            def _():
                mask_copy(b + nslot, slot).start()

        rd = lax.dot_general(ones, rowsum[...], NT, preferred_element_type=F32)[0:8]
        comp = jnp.zeros((8, 128), F32)
        for j in range(groups):
            comp = jnp.where(sub8 == j, rd[:, j * 128:(j + 1) * 128], comp)
        deg[pl.ds(pl.multiple_of(i * groups, groups), groups), :] = comp

    npair = users // pair
    per = npair // 4
    drows = deg.shape[0] // 4

    def deg_copy(d, p):
        sl = pl.ds(p * drows, drows)
        return remote(deg.at[sl], rdeg.at[d, sl], deg_s.at[d, p], deg_r.at[d, p], dev((nx, ny, nd)[d]))

    for p in range(4):
        def read_body(i, carry):
            read_pair(p * per + i)
            return carry

        lax.fori_loop(0, per, read_body, 0)
        for d in range(3):
            deg_copy(d, p).start()
        if p == 3:
            remote(col, rcol, col_sem.at[0], col_sem.at[1], partner).start()
        if p == 1:
            for hh in range(2):
                ag0(hh, hh).wait_recv()
                fw0(hh).start()
    ic.wait()
    items[0, :, 0:nhalf] = ei_half[0]
    items[0, :, nhalf:] = ei_half[1]
    remote(col, rcol, col_sem.at[0], col_sem.at[1], partner).wait()
    dv = jnp.sum(col[...] + rcol[...], axis=0, keepdims=True)
    sv[...] = jnp.broadcast_to(lax.rsqrt(jnp.maximum(dv, 1.0)), sv.shape)
    for d in range(3):
        for p in range(4):
            deg_copy(d, p).wait()
    du = deg[...] + rdeg[0] + rdeg[1] + rdeg[2]
    su[...] = lax.rsqrt(jnp.maximum(du, 1.0))

    def row_of(shard_id, hh, k):
        return pl.multiple_of(shard_id * shard + hh * half + k * width, width)

    def build(row0):
        g0 = row0 // 128
        for g in range(width // 128):
            sc = jnp.broadcast_to(su[pl.ds(g0 + g, 1), :], (128, 128)).T
            rows = pl.ds(pl.multiple_of(row0 + g * 128, 128), 128)
            for j in range(nitem // 128):
                cols = slice(j * 128, (j + 1) * 128)
                adj[rows, cols] = adj[rows, cols] * (sc * sv[0:1, cols]).astype(BF16)

    def send1(hh, k, t):
        nb = (1 - hh) * nx + hh * ny
        return remote(part.at[hh, k, t], recv1.at[hh, k, t], s1.at[hh, k, t], r1.at[hh, k, t], dev(nb))

    def send2(hh, k):
        nb = (1 - hh) * ny + hh * nx
        return remote(part.at[hh, k, 2], recv2.at[hh, k], s2.at[hh, k], r2.at[hh, k], dev(nb))

    def ag(j, d, hh, k):
        return remote(table.at[j, 0, hh, k], table.at[j, 1 + d, hh, k], ag_s.at[j, d, hh, k], ag_r.at[j, d, hh, k],
                      dev(nx if d == 0 else ny))

    def fw(j, hh, k):
        return remote(table.at[j, 1 + hh, hh, k], table.at[j, 3, hh, k], fw_s.at[j, hh, k], fw_r.at[j, hh, k],
                      dev(ny if hh == 0 else nx))

    def product(j, k):
        if j > 0:
            for hh in range(2):
                for t in range(2):
                    send1(hh, k, t).wait_send()
                send2(hh, k).wait_send()

        def body(i, carry):
            t = i // 2
            hh = i % 2
            fa = 1 - t // 2
            fb = 1 - t % 2
            fx = fa * (1 - hh) + fb * hh
            fy = fb * (1 - hh) + fa * hh
            row0 = row_of(flip(y, fy) * 2 + flip(x, fx), hh, k)
            if j == 0:
                build(row0)
            part[hh, k, t] = lax.dot_general(items[j], adj[pl.ds(row0, width), :], NT, preferred_element_type=F32)

            @pl.when(t < 2)
            def _():
                send1(hh, k, t).start()

            return carry

        lax.fori_loop(0, 8, body, 0)

    def step2(k):
        for hh in range(2):
            send1(hh, k, 0).wait_recv()
            part[hh, k, 2] = part[hh, k, 2] + recv1[hh, k, 0]
            send2(hh, k).start()

    def last(j, k):
        for hh in range(2):
            send1(hh, k, 1).wait_recv()
            send2(hh, k).wait_recv()
            res = (part[hh, k, 3] + recv1[hh, k, 1] + recv2[hh, k]).astype(BF16)
            if j + 1 < LAYERS:
                table[j + 1, 0, hh, k] = res
                ag(j + 1, hh, hh, k).start()
                ag(j + 1, 1 - hh, hh, k).start()
            else:
                tot = table[0, 0, hh, k].astype(F32) + table[1, 0, hh, k].astype(F32)
                tot = (tot + table[2, 0, hh, k].astype(F32)) + res.astype(F32)
                o = (tot * (1.0 / (LAYERS + 1))).T.astype(BF16)
                rows = pl.ds(hh * half + k * width, width)
                ubuf[rows, :] = o
                ucopy(hh, k).start()
                base = (r * 4 + c) * shard + hh * half + k * width
                ids = lax.broadcasted_iota(jnp.int32, (triples.shape[0], width), 1) + base
                hot = jnp.where(triples[:, 0:1] == ids, 1.0, 0.0).astype(BF16)
                picks[...] += jnp.dot(hot, o, preferred_element_type=F32)

    def ucopy(hh, k):
        rows = pl.ds(hh * half + k * width, width)
        return pltpu.make_async_copy(ubuf.at[rows], out_user.at[rows], out_sem.at[hh, k])

    def forward(j, k):
        for hh in range(2):
            ag(j + 1, hh, hh, k).wait_recv()
            fw(j + 1, hh, k).start()

    def gather_item(j, k):
        if j == 0:
            if k == 0:
                for hh in range(2):
                    ag0(1 - hh, hh).wait_recv()
                    fw0(hh).wait_recv()
        else:
            for hh in range(2):
                ag(j, 1 - hh, hh, k).wait_recv()
                fw(j, hh, k).wait_recv()

        def body(i, carry):
            q = i // 2
            hh = i % 2
            row0 = row_of(flip(y, q // 2) * 2 + flip(x, q % 2), hh, k)
            acc[...] += jnp.dot(table[j, q, hh, k], adj[pl.ds(row0, width), :], preferred_element_type=F32)
            return carry

        lax.fori_loop(0, 8, body, 0)

    def acc_copy(j):
        return remote(acc, racc.at[j], acc_s.at[j], acc_r.at[j], partner)

    def item_next(j):
        acc_copy(j).wait()
        items[j + 1] = (acc[...] + racc[j]).astype(BF16)
        if j + 1 < LAYERS:
            acc[...] = jnp.zeros_like(acc)

    acc[...] = jnp.zeros_like(acc)
    picks[...] = jnp.zeros_like(picks)

    total = LAYERS * NC
    for g in range(total + 2):
        j, k = g // NC, g % NC
        if g < total:
            product(j, k)
            if j == 0:
                gather_item(j, k)
        if g == NC - 1:
            acc_copy(0).start()
        if 0 <= g - 1 < total:
            step2((g - 1) % NC)
        if 0 <= g - 2 < total:
            last((g - 2) // NC, (g - 2) % NC)
        if 0 <= g - 3 < total and (g - 3) // NC + 1 < LAYERS:
            forward((g - 3) // NC, (g - 3) % NC)
        if g < total and j > 0:
            gather_item(j, k)
            if k == NC - 1:
                acc_copy(j).start()
        if g < total and k == NC - 1 and j + 1 < LAYERS:
            item_next(j)
        if g == total:
            item_next(LAYERS - 1)
            tot = items[0].astype(F32) + items[1].astype(F32)
            tot = (tot + items[2].astype(F32)) + items[3].astype(F32)
            o = (tot * (1.0 / (LAYERS + 1))).T.astype(BF16)
            ibuf[...] = o
            pltpu.make_async_copy(ibuf.at[pl.ds(r * nhalf, nhalf)], out_item, in_sem.at[0]).start()
            ids = lax.broadcasted_iota(jnp.int32, (triples.shape[0], nitem), 1) + c * nitem
            for n in range(2):
                hot = jnp.where(triples[:, n + 1:n + 2] == ids, 1.0, 0.0).astype(BF16)
                rpicks[0, n] = jnp.dot(hot, o, preferred_element_type=F32).astype(BF16)
            for d in range(3):
                pick_copy(d).start()
        if g + 1 == total:
            def pick_copy(d):
                return remote(rpicks.at[0], rpicks.at[1 + d], pick_s.at[d], pick_r.at[d], dev((nx, ny, nd)[d]))

    for d in range(3):
        pick_copy(d).wait()
    row_p = rpicks[0, 0].astype(F32)
    row_n = rpicks[0, 1].astype(F32)
    for d in range(3):
        row_p = row_p + rpicks[1 + d, 0].astype(F32)
        row_n = row_n + rpicks[1 + d, 1].astype(F32)
    margin = (jnp.sum(picks[...] * row_p, axis=1, keepdims=True)
              - jnp.sum(picks[...] * row_n, axis=1, keepdims=True))
    neg = -margin
    soft = jnp.maximum(neg, 0.0) + jnp.log1p(jnp.exp(-jnp.abs(neg)))
    me = r * 4 + c
    lid = triples[:, 0:1] - me * shard
    soft = jnp.where((lid >= 0) & (lid < shard), soft, 0.0)
    lbuf[me] = jnp.broadcast_to(jnp.sum(soft, axis=0, keepdims=True), (8, 128))

    def loss_copy(n, dc, dr):
        return remote(lbuf.at[me], lbuf.at[me], loss_s.at[n], loss_r.at[n], {"col": dc, "row": dr})

    others = [(nx, r), (ny, r), (nd, r), (c, 1 - r), (nx, 1 - r), (ny, 1 - r), (nd, 1 - r)]
    for n, (dc, dr) in enumerate(others):
        loss_copy(n, dc, dr).start()
    for n, (dc, dr) in enumerate(others):
        loss_copy(n, dc, dr).wait()
    tot = lbuf[0]
    for n in range(1, 8):
        tot = tot + lbuf[n]
    loss[...] = tot[0:1, 0:1] * (1.0 / triples.shape[0])

    for hh in range(2):
        for k in range(NC):
            ucopy(hh, k).wait()
            for t in range(2):
                send1(hh, k, t).wait_send()
            send2(hh, k).wait_send()
            for j in range(1, LAYERS):
                ag(j, 0, hh, k).wait_send()
                ag(j, 1, hh, k).wait_send()
                fw(j, hh, k).wait_send()
        ag0(0, hh).wait_send()
        ag0(1, hh).wait_send()
        fw0(hh).wait_send()
    pltpu.make_async_copy(ibuf.at[pl.ds(r * nhalf, nhalf)], out_item, in_sem.at[0]).wait()


def solution(mesh):
    def local_prog(mask_blk, user_shard, item_shard, triples):
        users, nitem = mask_blk.shape
        shard, dim = user_shard.shape
        trip = triples.shape[0]
        width = shard // 2 // NC
        hbm = pl.BlockSpec(memory_space=pl.ANY)
        vmem = pl.BlockSpec(memory_space=pltpu.VMEM)
        dma = pltpu.SemaphoreType.DMA
        scratch = [
            pltpu.VMEM((users, nitem), BF16),
            pltpu.VMEM((4, 512, nitem), jnp.int32),
            pltpu.VMEM((2, NC, 4, dim, width), F32),
            pltpu.VMEM((2, NC, 2, dim, width), F32),
            pltpu.VMEM((2, NC, dim, width), F32),
            pltpu.VMEM((LAYERS, 4, 2, NC, dim, width), BF16),
            pltpu.VMEM((dim, nitem), F32),
            pltpu.VMEM((LAYERS, dim, nitem), F32),
            pltpu.VMEM((LAYERS + 1, dim, nitem), BF16),
            pltpu.VMEM((shard, dim), BF16),
            pltpu.VMEM((nitem // 2, dim), BF16),
            pltpu.VMEM((2, dim, nitem // 2), BF16),
            pltpu.VMEM((1024, 128), BF16),
            pltpu.VMEM((users // 128, 128), F32),
            pltpu.VMEM((3, users // 128, 128), F32),
            pltpu.VMEM((8, nitem), F32),
            pltpu.VMEM((8, nitem), F32),
            pltpu.VMEM((users // 128, 128), F32),
            pltpu.VMEM((8, nitem), F32),
            pltpu.VMEM((shard, dim), BF16),
            pltpu.VMEM((nitem, dim), BF16),
            pltpu.VMEM((trip, dim), F32),
            pltpu.VMEM((4, 2, trip, dim), BF16),
            pltpu.VMEM((8, 8, 128), F32),
            dma((4,)), dma((2,)), dma((2, NC)), dma((2,)),
            dma((3, 4)), dma((3, 4)), dma((2,)),
            dma((2, 2)), dma((2, 2)), dma((2,)), dma((2,)),
            dma((2, NC, 2)), dma((2, NC, 2)), dma((2, NC)), dma((2, NC)),
            dma((LAYERS, 2, 2, NC)), dma((LAYERS, 2, 2, NC)),
            dma((LAYERS, 2, NC)), dma((LAYERS, 2, NC)),
            dma((LAYERS,)), dma((LAYERS,)),
            dma((3,)), dma((3,)), dma((7,)), dma((7,)),
        ]
        out_user, out_item, loss = pl.pallas_call(
            kernel,
            out_shape=(jax.ShapeDtypeStruct((shard, dim), BF16),
                       jax.ShapeDtypeStruct((nitem // 2, dim), BF16),
                       jax.ShapeDtypeStruct((1, 1), F32)),
            in_specs=[hbm, hbm, hbm, vmem],
            out_specs=(hbm, hbm, vmem),
            scratch_shapes=scratch,
            compiler_params=pltpu.CompilerParams(collective_id=0, has_side_effects=True,
                                                 vmem_limit_bytes=67043328),
        )(mask_blk, user_shard, item_shard, triples)
        return out_user, out_item, loss[0, 0]

    return jax.shard_map(local_prog, mesh=mesh, in_specs=(P("row", "col"), P(("row", "col"), None), P(("col", "row"), None), P(None, None)),
                         out_specs=(P(("row", "col"), None), P(("col", "row"), None), P()), check_vma=False)
```

```python
import functools

import jax
import jax.numpy as jnp
from jax import lax
from jax.experimental import pallas as pl
from jax.experimental.pallas import tpu as pltpu
from jax.sharding import PartitionSpec as P

LAYERS = 3
NC = 4
MESH = pl.DeviceIdType.MESH
F32 = jnp.float32
BF16 = jnp.bfloat16
NT = (((1,), (1,)), ((), ()))


def flip(v, f):
    return v + f - 2 * v * f


def kernel(mask, emb_user, emb_item, triples, out, loss,
           adj, ring, part, recv1, recv2, table, acc, racc, items, ei_half, trip,
           rowsum, deg, rdeg, col, rcol, su, sv, ubuf, ibuf, picks, rpicks, lbuf,
           ring_sem, in_sem, item_sem, deg_s, deg_r, col_sem, ag0_s, ag0_r, s1, r1, s2, r2, ag_s, ag_r, acc_s, acc_r,
           pick_sem, loss_sem):
    users, nitem = mask.shape
    shard = users // 4
    half = shard // 2
    width = half // NC
    nhalf = nitem // 2
    ntrip = triples.shape[1]
    c = lax.axis_index("col")
    r = lax.axis_index("row")
    x = c % 2
    y = c // 2
    nx = y * 2 + 1 - x
    ny = (1 - y) * 2 + x
    nd = (1 - y) * 2 + 1 - x

    def dev(col_id):
        return {"col": col_id, "row": r}

    partner = {"col": c, "row": 1 - r}

    def remote(src, dst, ss, rs, device):
        return pltpu.make_async_remote_copy(src_ref=src, dst_ref=dst, send_sem=ss, recv_sem=rs,
                                            device_id=device, device_id_type=MESH)

    def wait_bytes(ref, sem):
        pltpu.make_async_copy(ref, ref, sem).wait()

    blk = ring.shape[1]
    nslot = ring.shape[0]
    nblk = users // blk

    def mask_row(b):
        q = b * blk // width
        return (q % 8 // 2) * shard + (q % 2) * half + (q // 8) * width + (b * blk) % width

    def mask_copy(b, slot):
        rows = pl.ds(pl.multiple_of(mask_row(b), blk), blk)
        return pltpu.make_async_copy(mask.at[rows], ring.at[slot], ring_sem.at[slot])

    def user_in(hh, k):
        cols = pl.ds(hh * half + k * width, width)
        return pltpu.make_async_copy(emb_user.at[:, cols], table.at[0, 0, hh, k], in_sem.at[0])

    for hh in range(2):
        for k in range(NC):
            user_in(hh, k).start()
    ci = pltpu.make_async_copy(emb_item, ei_half.at[r], in_sem.at[1])
    ct = pltpu.make_async_copy(triples, trip, in_sem.at[2])
    ci.start()
    ct.start()
    for b in range(nslot):
        mask_copy(b, b).start()

    barrier = pltpu.get_barrier_semaphore()
    for dc in (c, nx, ny, nd):
        for dr in (r, 1 - r):
            if dc is c and dr is r:
                continue
            pl.semaphore_signal(barrier, inc=1, device_id={"col": dc, "row": dr}, device_id_type=MESH)

    ic = remote(ei_half.at[r], ei_half.at[r], item_sem.at[0], item_sem.at[1], partner)

    def ag0(d, hh):
        return remote(table.at[0, 0, hh], table.at[0, 1 + d, hh], ag0_s, ag0_r.at[hh if d == hh else 2],
                      dev(nx if d == 0 else ny))

    def fw0(hh, part_id):
        ks = pl.ds(part_id * (NC // 2), NC // 2)
        return remote(table.at[0, 1 + hh, hh, ks], table.at[0, 3, hh, ks], ag0_s, ag0_r.at[2 + part_id],
                      dev(ny if hh == 0 else nx))

    def share_tables():
        wait_bytes(table.at[0, 0], in_sem.at[0])
        ci.wait()
        ct.wait()
        pl.semaphore_wait(barrier, 7)
        for d, hh in ((0, 0), (1, 1), (0, 1), (1, 0)):
            ag0(d, hh).start()
        ic.start()

    strip = 32
    col[...] = jnp.zeros_like(col)
    ones = jnp.ones((16, 128), BF16)
    sub8 = lax.broadcasted_iota(jnp.int32, (8, 128), 0)
    pair = 2 * width
    nsub = pair // blk
    groups = pair // 128

    def read_pair(i):
        for u in range(nsub):
            b = i * nsub + u
            slot = (i % (nslot // nsub)) * nsub + u
            arow = mask_row(b)
            mask_copy(b, slot).wait()

            def strips(q, colacc):
                r0 = pl.multiple_of(q * strip, strip)
                m = ring[slot, pl.ds(r0, strip), :]
                mb = m.astype(F32).astype(BF16)
                adj[pl.ds(pl.multiple_of(arow + q * strip, strip), strip), :] = mb
                rsum = mb[:, 0:128]
                for j in range(1, nitem // 128):
                    rsum = rsum + mb[:, j * 128:(j + 1) * 128]
                rowsum[pl.ds(pl.multiple_of(u * blk + q * strip, strip), strip), :] = rsum
                for j in range(strip // 8):
                    colacc = colacc + m[j * 8:(j + 1) * 8, :]
                return colacc

            colacc = lax.fori_loop(0, blk // strip, strips, jnp.zeros((8, nitem), jnp.int32))
            col[...] += colacc.astype(F32)

            @pl.when(b + nslot < nblk)
            def _():
                mask_copy(b + nslot, slot).start()

        rd = lax.dot_general(ones, rowsum[...], NT, preferred_element_type=F32)[0:8]
        comp = jnp.zeros((8, 128), F32)
        for j in range(groups):
            comp = jnp.where(sub8 == j, rd[:, j * 128:(j + 1) * 128], comp)
        deg[pl.ds(pl.multiple_of(i * groups, groups), groups), :] = comp

    npair = users // pair
    per = npair // 4
    drows = deg.shape[0] // 4

    def deg_copy(d, p):
        sl = pl.ds(p * drows, drows)
        return remote(deg.at[sl], rdeg.at[d, sl], deg_s, deg_r.at[p], dev((nx, ny, nd)[d]))

    for p in range(4):
        def read_body(i, carry):
            read_pair(p * per + i)
            return carry

        if p == 0:
            lax.fori_loop(0, per - 1, read_body, 0)
            share_tables()
            lax.fori_loop(per - 1, per, read_body, 0)
        elif p == 2:
            lax.fori_loop(0, per // 2, read_body, 0)
            for hh in range(2):
                ag0(hh, hh).wait_recv()
                fw0(hh, 0).start()
            lax.fori_loop(per // 2, per, read_body, 0)
        else:
            lax.fori_loop(0, per, read_body, 0)
        if p == 3:
            remote(col, rcol, col_sem.at[0], col_sem.at[1], partner).start()
        for d in range(3):
            deg_copy(d, p).start()
        if p == 3:
            for hh in range(2):
                fw0(hh, 1).start()
    ic.wait()
    items[0, :, 0:nhalf] = ei_half[0]
    items[0, :, nhalf:] = ei_half[1]
    remote(col, rcol, col_sem.at[0], col_sem.at[1], partner).wait()
    dv = jnp.sum(col[...] + rcol[...], axis=0, keepdims=True)
    sv[...] = jnp.broadcast_to(lax.rsqrt(jnp.maximum(dv, 1.0)), sv.shape)

    def row_of(shard_id, hh, k):
        return pl.multiple_of(shard_id * shard + hh * half + k * width, width)

    def user_scale(k):
        sl = pl.ds(k * drows, drows)
        wait_bytes(rdeg.at[:, sl], deg_r.at[k])
        du = deg[sl] + rdeg[0, sl] + rdeg[1, sl] + rdeg[2, sl]
        su[sl] = lax.rsqrt(jnp.maximum(du, 1.0))

    def build(row0, g0):
        for g in range(width // 128):
            sc = jnp.broadcast_to(su[pl.ds(g0 + g, 1), :], (128, 128)).T
            rows = pl.ds(pl.multiple_of(row0 + g * 128, 128), 128)
            for j in range(nitem // 128):
                cols = slice(j * 128, (j + 1) * 128)
                adj[rows, cols] = adj[rows, cols] * (sc * sv[0:1, cols]).astype(BF16)

    def send1(hh, k, t):
        nb = (1 - hh) * nx + hh * ny
        return remote(part.at[hh, k, t], recv1.at[hh, k, t], s1.at[hh, k], r1.at[hh, k, t], dev(nb))

    def send2(hh, k):
        nb = (1 - hh) * ny + hh * nx
        return remote(part.at[hh, k, 2], recv2.at[hh, k], s2.at[hh, k], r2.at[hh, k], dev(nb))

    def ag(j, d, hh, k):
        return remote(table.at[j, 0, hh, k], table.at[j, 1 + d, hh, k], ag_s.at[j - 1],
                      ag_r.at[j - 1, 0 if d == hh else 1, k],
                      dev(nx if d == 0 else ny))

    def fw(j, hh, k):
        return remote(table.at[j, 1 + hh, hh, k], table.at[j, 3, hh, k], ag_s.at[j - 1], ag_r.at[j - 1, 1, k],
                      dev(ny if hh == 0 else nx))

    def sends_done(k):
        for hh in range(2):
            wait_bytes(part.at[hh, k, pl.ds(0, 2)], s1.at[hh, k])
            send2(hh, k).wait_send()

    def product(j, k):
        if j > 0:
            sends_done(k)
        else:
            user_scale(k)

        def body(i, carry):
            t = i // 2
            hh = i % 2
            fa = 1 - t // 2
            fb = 1 - t % 2
            fx = fa * (1 - hh) + fb * hh
            fy = fb * (1 - hh) + fa * hh
            owner = flip(y, fy) * 2 + flip(x, fx)
            row0 = row_of(owner, hh, k)
            if j == 0:
                build(row0, ((k * 4 + owner) * 2 + hh) * (width // 128))
            part[hh, k, t] = lax.dot_general(items[j], adj[pl.ds(row0, width), :], NT, preferred_element_type=F32)

            @pl.when(t < 2)
            def _():
                send1(hh, k, t).start()

            return carry

        lax.fori_loop(0, 8, body, 0)

    def step2(k):
        for hh in range(2):
            send1(hh, k, 0).wait_recv()
            part[hh, k, 2] = part[hh, k, 2] + recv1[hh, k, 0]
            send2(hh, k).start()

    def last(j, k):
        for hh in range(2):
            send1(hh, k, 1).wait_recv()
            send2(hh, k).wait_recv()
            res = (part[hh, k, 3] + recv1[hh, k, 1] + recv2[hh, k]).astype(BF16)
            if j + 1 < LAYERS:
                table[j + 1, 0, hh, k] = res
                ag(j + 1, hh, hh, k).start()
                ag(j + 1, 1 - hh, hh, k).start()
            else:
                tot = table[0, 0, hh, k].astype(F32) + table[1, 0, hh, k].astype(F32)
                tot = (tot + table[2, 0, hh, k].astype(F32)) + res.astype(F32)
                o = (tot * (1.0 / (LAYERS + 1))).astype(BF16)
                ubuf[hh, k] = o
                ucopy(hh, k).start()
                base = (r * 4 + c) * shard + hh * half + k * width
                ids = lax.broadcasted_iota(jnp.int32, (width, ntrip), 0) + base
                hot = jnp.where(trip[0:1, :] == ids, 1.0, 0.0).astype(BF16)
                picks[...] += jnp.dot(o, hot, preferred_element_type=F32)

    def ucopy(hh, k):
        cols = pl.ds(hh * half + k * width, width)
        return pltpu.make_async_copy(ubuf.at[hh, k], out.at[:, cols], in_sem.at[0])

    def forward(j, k):
        wait_bytes(table.at[j + 1, pl.ds(0, 2), 0, k], ag_r.at[j, 0, k])
        for hh in range(2):
            fw(j + 1, hh, k).start()

    def gather_item(j, k):
        if j == 0:
            if k == 0:
                wait_bytes(table.at[0, pl.ds(0, 3), 0], ag0_r.at[2])
            if k == NC // 2:
                wait_bytes(table.at[0, 3, 0], ag0_r.at[3])
        else:
            wait_bytes(table.at[j, pl.ds(0, 4), 0, k], ag_r.at[j - 1, 1, k])

        def body(i, carry):
            q = i // 2
            hh = i % 2
            row0 = row_of(flip(y, q // 2) * 2 + flip(x, q % 2), hh, k)
            acc[...] += jnp.dot(table[j, q, hh, k], adj[pl.ds(row0, width), :], preferred_element_type=F32)
            return carry

        lax.fori_loop(0, 8, body, 0)

    def acc_copy(j):
        return remote(acc, racc.at[j], acc_s.at[j], acc_r.at[j], partner)

    def item_next(j):
        acc_copy(j).wait()
        items[j + 1] = (acc[...] + racc[j]).astype(BF16)
        if j + 1 < LAYERS:
            acc[...] = jnp.zeros_like(acc)

    def pick_copy(d):
        return remote(rpicks.at[0], rpicks.at[1 + d], pick_sem.at[0], pick_sem.at[1], dev((nx, ny, nd)[d]))

    def finish_items():
        item_next(LAYERS - 1)
        tot = items[0].astype(F32) + items[1].astype(F32)
        tot = (tot + items[2].astype(F32)) + items[3].astype(F32)
        o = (tot * (1.0 / (LAYERS + 1))).astype(BF16)
        ibuf[0] = o[:, 0:nhalf]
        ibuf[1] = o[:, nhalf:]
        pltpu.make_async_copy(ibuf.at[r], out.at[:, pl.ds(shard, nhalf)], in_sem.at[1]).start()
        ids = lax.broadcasted_iota(jnp.int32, (nitem, ntrip), 0) + c * nitem
        for n in range(2):
            hot = jnp.where(trip[n + 1:n + 2, :] == ids, 1.0, 0.0).astype(BF16)
            rpicks[0, n] = jnp.dot(o, hot, preferred_element_type=F32).astype(BF16)
        for d in range(3):
            pick_copy(d).start()

    acc[...] = jnp.zeros_like(acc)
    picks[...] = jnp.zeros_like(picks)

    total = LAYERS * NC
    for g in range(total + 2):
        j, k = g // NC, g % NC
        edge = k == 0 and j > 0
        if g < total and not edge:
            product(j, k)
        if j == 0 and k >= NC // 2:
            gather_item(0, k - NC // 2)
        if g == NC:
            for kk in range(NC // 2, NC):
                gather_item(0, kk)
            acc_copy(0).start()
        if 0 <= g - 1 < total:
            step2((g - 1) % NC)
        if g == total:
            finish_items()
        if 0 <= g - 2 < total:
            last((g - 2) // NC, (g - 2) % NC)
        if 0 <= g - 3 < total and (g - 3) // NC + 1 < LAYERS:
            forward((g - 3) // NC, (g - 3) % NC)
        if g < total and edge:
            item_next(j - 1)
            product(j, k)
        if g < total and j > 0:
            gather_item(j, k)
            if k == NC - 1:
                acc_copy(j).start()

    wait_bytes(rpicks.at[pl.ds(1, 3)], pick_sem.at[1])
    row_p = rpicks[0, 0].astype(F32)
    row_n = rpicks[0, 1].astype(F32)
    for d in range(3):
        row_p = row_p + rpicks[1 + d, 0].astype(F32)
        row_n = row_n + rpicks[1 + d, 1].astype(F32)
    margin = (jnp.sum(picks[...] * row_p, axis=0, keepdims=True)
              - jnp.sum(picks[...] * row_n, axis=0, keepdims=True))
    neg = -margin
    soft = jnp.maximum(neg, 0.0) + jnp.log1p(jnp.exp(-jnp.abs(neg)))
    me = r * 4 + c
    lid = trip[0:1, :] - me * shard
    soft = jnp.where((lid >= 0) & (lid < shard), soft, 0.0)
    lbuf[me] = jnp.broadcast_to(jnp.sum(soft, axis=1, keepdims=True), (8, 128))

    def loss_copy(n, dc, dr):
        return remote(lbuf.at[me], lbuf.at[me], loss_sem.at[0], loss_sem.at[1], {"col": dc, "row": dr})

    others = [(nx, r), (ny, r), (nd, r), (c, 1 - r), (nx, 1 - r), (ny, 1 - r), (nd, 1 - r)]
    for n, (dc, dr) in enumerate(others):
        loss_copy(n, dc, dr).start()
    wait_bytes(lbuf.at[pl.ds(0, 7)], loss_sem.at[1])
    tot = lbuf[0]
    for n in range(1, 8):
        tot = tot + lbuf[n]
    loss[...] = tot[0:1, 0:1] * (1.0 / ntrip)

    wait_bytes(ubuf, in_sem.at[0])
    for k in range(NC):
        sends_done(k)
    for j in range(1, LAYERS):
        wait_bytes(table.at[j, pl.ds(0, 3)], ag_s.at[j - 1])
    wait_bytes(table.at[0, pl.ds(0, 3)], ag0_s)
    wait_bytes(rdeg, deg_s)
    wait_bytes(rpicks.at[pl.ds(1, 3)], pick_sem.at[0])
    wait_bytes(lbuf.at[pl.ds(0, 7)], loss_sem.at[0])
    pltpu.make_async_copy(ibuf.at[r], out.at[:, pl.ds(shard, nhalf)], in_sem.at[1]).wait()


def solution(mesh):
    def local_prog(mask_blk, user_shard, item_shard, triples):
        users, nitem = mask_blk.shape
        shard, dim = user_shard.shape
        trip = triples.shape[0]
        width = shard // 2 // NC
        hbm = pl.BlockSpec(memory_space=pl.ANY)
        vmem = pl.BlockSpec(memory_space=pltpu.VMEM)
        dma = pltpu.SemaphoreType.DMA
        scratch = [
            pltpu.VMEM((users, nitem), BF16),
            pltpu.VMEM((8, 256, nitem), jnp.int32),
            pltpu.VMEM((2, NC, 4, dim, width), F32),
            pltpu.VMEM((2, NC, 2, dim, width), F32),
            pltpu.VMEM((2, NC, dim, width), F32),
            pltpu.VMEM((LAYERS, 4, 2, NC, dim, width), BF16),
            pltpu.VMEM((dim, nitem), F32),
            pltpu.VMEM((LAYERS, dim, nitem), F32),
            pltpu.VMEM((LAYERS + 1, dim, nitem), BF16),
            pltpu.VMEM((2, dim, nitem // 2), BF16),
            pltpu.VMEM((3, trip), jnp.int32),
            pltpu.VMEM((2 * width, 128), BF16),
            pltpu.VMEM((users // 128, 128), F32),
            pltpu.VMEM((3, users // 128, 128), F32),
            pltpu.VMEM((8, nitem), F32),
            pltpu.VMEM((8, nitem), F32),
            pltpu.VMEM((users // 128, 128), F32),
            pltpu.VMEM((8, nitem), F32),
            pltpu.VMEM((2, NC, dim, width), BF16),
            pltpu.VMEM((2, dim, nitem // 2), BF16),
            pltpu.VMEM((dim, trip), F32),
            pltpu.VMEM((4, 2, dim, trip), BF16),
            pltpu.VMEM((8, 8, 128), F32),
            dma((8,)), dma((3,)), dma((2,)), dma, dma((4,)), dma((2,)),
            dma, dma((4,)),
            dma((2, NC)), dma((2, NC, 2)), dma((2, NC)), dma((2, NC)),
            dma((LAYERS - 1,)), dma((LAYERS - 1, 2, NC)),
            dma((LAYERS,)), dma((LAYERS,)), dma((2,)), dma((2,)),
        ]
        out, loss = pl.pallas_call(
            kernel,
            out_shape=(jax.ShapeDtypeStruct((dim, shard + nitem // 2), BF16),
                       jax.ShapeDtypeStruct((1, 1), F32)),
            in_specs=[hbm, hbm, hbm, hbm],
            out_specs=(hbm, vmem),
            scratch_shapes=scratch,
            compiler_params=pltpu.CompilerParams(collective_id=0, has_side_effects=True,
                                                 vmem_limit_bytes=67043328),
        )(mask_blk, user_shard.T, item_shard.T, triples.T)
        return out[:, :shard].T, out[:, shard:].T, loss[0, 0]

    return jax.shard_map(local_prog, mesh=mesh, in_specs=(P("row", "col"), P(("row", "col"), None), P(("col", "row"), None), P(None, None)),
                         out_specs=(P(("row", "col"), None), P(("col", "row"), None), P()), check_vma=False)
```

```python
import functools

import jax
import jax.numpy as jnp
from jax import lax
from jax.experimental import pallas as pl
from jax.experimental.pallas import tpu as pltpu
from jax.sharding import PartitionSpec as P

LAYERS = 3
NC = 4
MESH = pl.DeviceIdType.MESH
F32 = jnp.float32
BF16 = jnp.bfloat16
NT = (((1,), (1,)), ((), ()))


def flip(v, f):
    return v + f - 2 * v * f


def kernel(mask, emb_user, emb_item, triples, out, loss,
           adj, ring, part, recv1, recv2, table, acc, racc, items, ei_half, trip,
           rowsum, deg, rdeg, dsum, col, rcol, su, sv, ubuf, ibuf, picks, rpicks, rows, tsum, hots, lbuf,
           ring_sem, in_sem, item_sem, deg_s, deg_r, col_sem, ag0_s, ag0_r, sent, r1, r2, ag_s, ag_r, acc_s, acc_r,
           pick_sem, loss_sem):
    users, nitem = mask.shape
    shard = users // 4
    half = shard // 2
    width = half // NC
    nhalf = nitem // 2
    ntrip = triples.shape[1]
    c = lax.axis_index("col")
    r = lax.axis_index("row")
    x = c % 2
    y = c // 2
    nx = y * 2 + 1 - x
    ny = (1 - y) * 2 + x
    nd = (1 - y) * 2 + 1 - x

    def dev(col_id):
        return {"col": col_id, "row": r}

    partner = {"col": c, "row": 1 - r}

    def remote(src, dst, ss, rs, device):
        return pltpu.make_async_remote_copy(src_ref=src, dst_ref=dst, send_sem=ss, recv_sem=rs,
                                            device_id=device, device_id_type=MESH)

    def wait_bytes(ref, sem):
        pltpu.make_async_copy(ref, ref, sem).wait()

    blk = ring.shape[1]
    nslot = ring.shape[0]
    nblk = users // blk

    def mask_row(b):
        q = b * blk // width
        return (q % 8 // 2) * shard + (q % 2) * half + (q // 8) * width + (b * blk) % width

    def mask_copy(b, slot):
        rows = pl.ds(pl.multiple_of(mask_row(b), blk), blk)
        return pltpu.make_async_copy(mask.at[rows], ring.at[slot], ring_sem.at[slot])

    for b in range(nslot):
        mask_copy(b, b).start()

    def user_cols(hh, k):
        return emb_user.at[:, pl.ds(hh * half + k * width, width)]

    def user_in(hh, k):
        return pltpu.make_async_copy(user_cols(hh, k), table.at[0, 0, hh, k], in_sem.at[0])

    for hh in range(2):
        for k in range(NC):
            user_in(hh, k).start()
    ci = pltpu.make_async_copy(emb_item, ei_half.at[r], in_sem.at[1])
    ct = pltpu.make_async_copy(triples, trip, in_sem.at[2])
    ci.start()
    ct.start()

    barrier = pltpu.get_barrier_semaphore()
    for dc in (c, nx, ny, nd):
        for dr in (r, 1 - r):
            if dc is c and dr is r:
                continue
            pl.semaphore_signal(barrier, inc=1, device_id={"col": dc, "row": dr}, device_id_type=MESH)

    ic = remote(ei_half.at[r], ei_half.at[r], item_sem.at[0], item_sem.at[1], partner)

    def ag0_start(d, hh):
        for k in range(NC):
            remote(user_cols(hh, k), table.at[0, 1 + d, hh, k], ag0_s, ag0_r.at[hh if d == hh else 2],
                   dev(nx if d == 0 else ny)).start()

    def fw0(hh, part_id):
        ks = pl.ds(part_id * (NC // 2), NC // 2)
        return remote(table.at[0, 1 + hh, hh, ks], table.at[0, 3, hh, ks], ag0_s, ag0_r.at[2 + part_id],
                      dev(ny if hh == 0 else nx))

    def share_tables():
        pl.semaphore_wait(barrier, 7)
        for hh in range(2):
            ag0_start(hh, hh)

    strip = 64
    col[...] = jnp.zeros_like(col)
    ones = jnp.ones((16, 128), BF16)
    sub8 = lax.broadcasted_iota(jnp.int32, (8, 128), 0)
    pair = 2 * width
    nsub = pair // blk
    groups = pair // 128

    def read_pair(i):
        turn = i % (nslot // nsub)
        for u in range(nsub):
            b = i * nsub + u
            slot = turn * nsub + u
            arow = mask_row(b)
            mask_copy(b, slot).wait()

            def strips(q, colacc):
                r0 = pl.multiple_of(q * strip, strip)
                m = ring[slot, pl.ds(r0, strip), :]
                mb = m.astype(F32).astype(BF16)
                adj[pl.ds(pl.multiple_of(arow + q * strip, strip), strip), :] = mb
                rsum = mb[:, 0:128]
                for j in range(1, nitem // 128):
                    rsum = rsum + mb[:, j * 128:(j + 1) * 128]
                rowsum[pl.ds(pl.multiple_of(u * blk + q * strip, strip), strip), :] = rsum
                for j in range(strip // 8):
                    colacc = colacc + m[j * 8:(j + 1) * 8, :]
                return colacc

            colacc = lax.fori_loop(0, blk // strip, strips, jnp.zeros((8, nitem), jnp.int32), unroll=2)
            col[...] += colacc.astype(F32)

            @pl.when(b + nslot < nblk)
            def _():
                mask_copy(b + nslot, slot).start()

        rd = lax.dot_general(ones, rowsum[...], NT, preferred_element_type=F32)[0:8]
        comp = jnp.zeros((8, 128), F32)
        for j in range(groups):
            comp = jnp.where(sub8 == j, rd[:, j * 128:(j + 1) * 128], comp)
        deg[pl.ds(pl.multiple_of(i * groups, groups), groups), :] = comp

    npair = users // pair
    per = npair // 4
    drows = deg.shape[0] // 4

    def deg_rows(p):
        return pl.ds(p * drows, drows)

    def deg_x(p):
        return remote(deg.at[deg_rows(p)], rdeg.at[0, deg_rows(p)], deg_s, deg_r.at[0, p], dev(nx))

    def deg_y(p):
        return remote(dsum.at[deg_rows(p)], rdeg.at[1, deg_rows(p)], deg_s, deg_r.at[1, p], dev(ny))

    def deg_turn(p):
        deg_x(p).wait_recv()
        dsum[deg_rows(p)] = deg[deg_rows(p)] + rdeg[0, deg_rows(p)]
        deg_y(p).start()

    for p in range(4):
        def read_body(i, carry):
            read_pair(p * per + i)
            return carry

        if p == 0:
            share_tables()
        cut = per // 2 if p >= 2 else 0
        if cut:
            lax.fori_loop(0, cut, read_body, 0)
            deg_turn(p - 2)
        if p == 2:
            for hh in range(2):
                wait_bytes(table.at[0, 1 + hh, hh], ag0_r.at[hh])
                fw0(hh, 0).start()
        if p == 3:
            for hh in range(2):
                fw0(hh, 1).start()
        lax.fori_loop(cut, per, read_body, 0)
        if p == 3:
            remote(col, rcol, col_sem.at[0], col_sem.at[1], partner).start()
        deg_x(p).start()
        if p == 0:
            for hh in range(2):
                ag0_start(1 - hh, hh)
            ci.wait()
            ct.wait()
            ic.start()
    wait_bytes(table.at[0, 0], in_sem.at[0])
    ic.wait()
    items[0, :, 0:nhalf] = ei_half[0]
    items[0, :, nhalf:] = ei_half[1]
    remote(col, rcol, col_sem.at[0], col_sem.at[1], partner).wait()
    dv = jnp.sum(col[...] + rcol[...], axis=0, keepdims=True)
    sv[...] = jnp.broadcast_to(lax.rsqrt(jnp.maximum(dv, 1.0)), sv.shape)

    def row_of(shard_id, hh, k):
        return pl.multiple_of(shard_id * shard + hh * half + k * width, width)

    def user_scale(k):
        sl = deg_rows(k)
        deg_y(k).wait_recv()
        su[sl] = lax.rsqrt(jnp.maximum(dsum[sl] + rdeg[1, sl], 1.0))

    def build(row0, g0):
        for g in range(width // 128):
            sc = jnp.broadcast_to(su[pl.ds(g0 + g, 1), :], (128, 128)).T
            rows = pl.ds(pl.multiple_of(row0 + g * 128, 128), 128)
            for j in range(nitem // 128):
                cols = slice(j * 128, (j + 1) * 128)
                adj[rows, cols] = adj[rows, cols] * (sc * sv[0:1, cols]).astype(BF16)

    def send1(hh, k, t):
        nb = (1 - hh) * nx + hh * ny
        return remote(part.at[hh, k, t], recv1.at[hh, k, t], sent.at[k], r1.at[hh, k, t], dev(nb))

    def send2(hh, k):
        nb = (1 - hh) * ny + hh * nx
        return remote(part.at[hh, k, 2], recv2.at[hh, k], sent.at[k], r2.at[hh, k], dev(nb))

    def ag(j, d, hh, k):
        return remote(table.at[j, 0, hh, k], table.at[j, 1 + d, hh, k], ag_s.at[j - 1],
                      ag_r.at[j - 1, 0 if d == hh else 1, k],
                      dev(nx if d == 0 else ny))

    def fw(j, hh, k):
        return remote(table.at[j, 1 + hh, hh, k], table.at[j, 3, hh, k], ag_s.at[j - 1], ag_r.at[j - 1, 1, k],
                      dev(ny if hh == 0 else nx))

    def sends_done(k):
        wait_bytes(part.at[0, pl.ds(0, 3), pl.ds(0, 2)], sent.at[k])

    def product(j, k):
        if j > 0:
            sends_done(k)
        else:
            if k < 2:
                deg_turn(2 + k)
            user_scale(k)

        def body(i, carry):
            t = i // 2
            hh = i % 2
            fa = 1 - t // 2
            fb = 1 - t % 2
            fx = fa * (1 - hh) + fb * hh
            fy = fb * (1 - hh) + fa * hh
            owner = flip(y, fy) * 2 + flip(x, fx)
            row0 = row_of(owner, hh, k)
            if j == 0:
                build(row0, ((k * 4 + owner) * 2 + hh) * (width // 128))
            part[hh, k, t] = lax.dot_general(items[j], adj[pl.ds(row0, width), :], NT, preferred_element_type=F32)

            @pl.when(t < 2)
            def _():
                send1(hh, k, t).start()

            return carry

        lax.fori_loop(0, 8, body, 0)

    def step2(k):
        for hh in range(2):
            send1(hh, k, 0).wait_recv()
            part[hh, k, 2] = part[hh, k, 2] + recv1[hh, k, 0]
            send2(hh, k).start()

    def last(j, k):
        if j + 1 < LAYERS:
            for hh in range(2):
                send1(hh, k, 1).wait_recv()
                send2(hh, k).wait_recv()
                table[j + 1, 0, hh, k] = (part[hh, k, 3] + recv1[hh, k, 1] + recv2[hh, k]).astype(BF16)
                ag(j + 1, hh, hh, k).start()
                ag(j + 1, 1 - hh, hh, k).start()
            return
        for hh in range(2):
            send1(hh, k, 1).wait_recv()
            part[hh, k, 3] = part[hh, k, 3] + recv1[hh, k, 1]
            tot = table[0, 0, hh, k].astype(F32) + table[1, 0, hh, k].astype(F32)
            tsum[hh] = tot + table[2, 0, hh, k].astype(F32)
            base = (r * 4 + c) * shard + hh * half + k * width
            ids = lax.broadcasted_iota(jnp.int32, (width, ntrip), 0) + base
            hots[hh] = jnp.where(trip[0:1, :] == ids, 1.0, 0.0).astype(BF16)
        for hh in range(2):
            send2(hh, k).wait_recv()
            res = (part[hh, k, 3] + recv2[hh, k]).astype(BF16)
            o = ((tsum[hh] + res.astype(F32)) * (1.0 / (LAYERS + 1))).astype(BF16)
            ubuf[hh, k] = o
            ucopy(hh, k).start()
            picks[...] += jnp.dot(o, hots[hh], preferred_element_type=F32)

    def ucopy(hh, k):
        cols = pl.ds(hh * half + k * width, width)
        return pltpu.make_async_copy(ubuf.at[hh, k], out.at[:, cols], in_sem.at[0])

    def forward(j, k):
        wait_bytes(table.at[j + 1, pl.ds(0, 2), 0, k], ag_r.at[j, 0, k])
        for hh in range(2):
            fw(j + 1, hh, k).start()

    def gather_item(j, k):
        if j == 0:
            if k == 0:
                wait_bytes(table.at[0, pl.ds(0, 3), 0], ag0_r.at[2])
            if k == NC // 2:
                wait_bytes(table.at[0, 3, 0], ag0_r.at[3])
        else:
            wait_bytes(table.at[j, pl.ds(0, 4), 0, k], ag_r.at[j - 1, 1, k])

        def body(i, carry):
            q = i // 2
            hh = i % 2
            row0 = row_of(flip(y, q // 2) * 2 + flip(x, q % 2), hh, k)
            acc[...] += jnp.dot(table[j, q, hh, k], adj[pl.ds(row0, width), :], preferred_element_type=F32)
            return carry

        lax.fori_loop(0, 8, body, 0)

    def acc_copy(j):
        return remote(acc, racc.at[j], acc_s, acc_r.at[j], partner)

    def item_next(j):
        acc_copy(j).wait()
        items[j + 1] = (acc[...] + racc[j]).astype(BF16)
        if j + 1 < LAYERS:
            acc[...] = jnp.zeros_like(acc)

    def pick_copy(d):
        return remote(rpicks.at[0], rpicks.at[1 + d], pick_sem.at[0], pick_sem.at[1], dev((nx, ny, nd)[d]))

    def rows_copy():
        return remote(rows.at[r], rows.at[r], pick_sem.at[2], pick_sem.at[3], partner)

    def pick_swap():
        wait_bytes(rpicks.at[pl.ds(1, 3)], pick_sem.at[1])
        row = rpicks[0].astype(F32)
        for d in range(3):
            row = row + rpicks[1 + d].astype(F32)
        rows[r] = row.astype(BF16)
        rows_copy().start()

    def finish_items():
        item_next(LAYERS - 1)
        tot = items[0].astype(F32) + items[1].astype(F32)
        tot = (tot + items[2].astype(F32)) + items[3].astype(F32)
        o = (tot * (1.0 / (LAYERS + 1))).astype(BF16)
        ibuf[0] = o[:, 0:nhalf]
        ibuf[1] = o[:, nhalf:]
        pltpu.make_async_copy(ibuf.at[r], out.at[:, pl.ds(shard, nhalf)], in_sem.at[1]).start()
        ids = lax.broadcasted_iota(jnp.int32, (nitem, ntrip), 0) + c * nitem
        hot = jnp.where(trip[pl.ds(1 + r, 1), :] == ids, 1.0, 0.0).astype(BF16)
        rpicks[0] = jnp.dot(o, hot, preferred_element_type=F32).astype(BF16)
        for d in range(3):
            pick_copy(d).start()

    acc[...] = jnp.zeros_like(acc)
    picks[...] = jnp.zeros_like(picks)

    total = LAYERS * NC
    for g in range(total + 2):
        j, k = g // NC, g % NC
        edge = k == 0 and j > 0
        if g < total and not edge:
            product(j, k)
        if j == 0 and k >= NC // 2:
            gather_item(0, k - NC // 2)
        if g == NC:
            for kk in range(NC // 2, NC):
                gather_item(0, kk)
            acc_copy(0).start()
        if g == total:
            finish_items()
        if 0 <= g - 1 < total:
            step2((g - 1) % NC)
        if g == total - 1:
            gather_item(j, k)
            acc_copy(j).start()
        if 0 <= g - 2 < total:
            last((g - 2) // NC, (g - 2) % NC)
        if g == total:
            pick_swap()
        if 0 <= g - 3 < total and (g - 3) // NC + 1 < LAYERS:
            forward((g - 3) // NC, (g - 3) % NC)
        if g < total and edge:
            item_next(j - 1)
            product(j, k)
        if g < total - 1 and j > 0:
            gather_item(j, k)
            if k == NC - 1:
                acc_copy(j).start()

    rows_copy().wait()
    row_p = rows[0].astype(F32)
    row_n = rows[1].astype(F32)
    margin = (jnp.sum(picks[...] * row_p, axis=0, keepdims=True)
              - jnp.sum(picks[...] * row_n, axis=0, keepdims=True))
    neg = -margin
    soft = jnp.maximum(neg, 0.0) + jnp.log1p(jnp.exp(-jnp.abs(neg)))
    me = r * 4 + c
    lid = trip[0:1, :] - me * shard
    soft = jnp.where((lid >= 0) & (lid < shard), soft, 0.0)
    lbuf[me] = jnp.broadcast_to(jnp.sum(soft, axis=1, keepdims=True), (8, 128))

    def loss_copy(n, dc, dr):
        return remote(lbuf.at[me], lbuf.at[me], loss_sem.at[0], loss_sem.at[1], {"col": dc, "row": dr})

    others = [(nx, r), (ny, r), (nd, r), (c, 1 - r), (nx, 1 - r), (ny, 1 - r), (nd, 1 - r)]
    for n, (dc, dr) in enumerate(others):
        loss_copy(n, dc, dr).start()
    wait_bytes(lbuf.at[pl.ds(0, 7)], loss_sem.at[1])
    tot = lbuf[0]
    for n in range(1, 8):
        tot = tot + lbuf[n]
    loss[...] = tot * (1.0 / ntrip)

    wait_bytes(ubuf, in_sem.at[0])
    for k in range(NC):
        sends_done(k)
    for j in range(1, LAYERS):
        wait_bytes(table.at[j, pl.ds(0, 3)], ag_s.at[j - 1])
    wait_bytes(table.at[0, pl.ds(0, 3)], ag0_s)
    wait_bytes(rdeg, deg_s)
    wait_bytes(rpicks.at[pl.ds(1, 3)], pick_sem.at[0])
    wait_bytes(lbuf.at[pl.ds(0, 7)], loss_sem.at[0])
    pltpu.make_async_copy(ibuf.at[r], out.at[:, pl.ds(shard, nhalf)], in_sem.at[1]).wait()


def split_kernel(both, one, out_user, out_item, out_one, buf, one_buf, one_val, in_sem, out_sem):
    shard = out_user.shape[1]
    step = shard // 4
    spans = [(n * step, step) for n in range(4)] + [(shard, out_item.shape[1])]
    loads = [pltpu.make_async_copy(both.at[:, pl.ds(o, w)], buf.at[:, pl.ds(o, w)], in_sem.at[n])
             for n, (o, w) in enumerate(spans)]
    stores = [pltpu.make_async_copy(buf.at[:, pl.ds(o, w)],
                                    out_user.at[:, pl.ds(o, w)] if o < shard else out_item, out_sem.at[n])
              for n, (o, w) in enumerate(spans)]
    loads.insert(0, pltpu.make_async_copy(one, one_buf, in_sem.at[5]))
    stores.insert(0, pltpu.make_async_copy(one_val, out_one, out_sem.at[5]))
    for cp in loads:
        cp.start()
    for n, (ld, st) in enumerate(zip(loads, stores)):
        ld.wait()
        if n == 0:
            one_val[...] = one_buf[0:1, 0:1]
        st.start()
    for st in stores:
        st.wait()


def solution(mesh):
    def local_prog(mask_blk, user_shard, item_shard, triples):
        users, nitem = mask_blk.shape
        shard, dim = user_shard.shape
        trip = triples.shape[0]
        width = shard // 2 // NC
        hbm = pl.BlockSpec(memory_space=pl.ANY)
        vmem = pl.BlockSpec(memory_space=pltpu.VMEM)
        dma = pltpu.SemaphoreType.DMA
        scratch = [
            pltpu.VMEM((users, nitem), BF16),
            pltpu.VMEM((12, 256, nitem), jnp.int32),
            pltpu.VMEM((2, NC, 4, dim, width), F32),
            pltpu.VMEM((2, NC, 2, dim, width), F32),
            pltpu.VMEM((2, NC, dim, width), F32),
            pltpu.VMEM((LAYERS, 4, 2, NC, dim, width), BF16),
            pltpu.VMEM((dim, nitem), F32),
            pltpu.VMEM((LAYERS, dim, nitem), F32),
            pltpu.VMEM((LAYERS + 1, dim, nitem), BF16),
            pltpu.VMEM((2, dim, nitem // 2), BF16),
            pltpu.VMEM((3, trip), jnp.int32),
            pltpu.VMEM((2 * width, 128), BF16),
            pltpu.VMEM((users // 128, 128), F32),
            pltpu.VMEM((2, users // 128, 128), F32),
            pltpu.VMEM((users // 128, 128), F32),
            pltpu.VMEM((8, nitem), F32),
            pltpu.VMEM((8, nitem), F32),
            pltpu.VMEM((users // 128, 128), F32),
            pltpu.VMEM((8, nitem), F32),
            pltpu.VMEM((2, NC, dim, width), BF16),
            pltpu.VMEM((2, dim, nitem // 2), BF16),
            pltpu.VMEM((dim, trip), F32),
            pltpu.VMEM((4, dim, trip), BF16),
            pltpu.VMEM((2, dim, trip), BF16),
            pltpu.VMEM((2, dim, width), F32),
            pltpu.VMEM((2, width, trip), BF16),
            pltpu.VMEM((8, 8, 128), F32),
            dma((12,)), dma((3,)), dma((2,)), dma, dma((2, 4)), dma((2,)),
            dma, dma((4,)),
            dma((NC,)), dma((2, NC, 2)), dma((2, NC)),
            dma((LAYERS - 1,)), dma((LAYERS - 1, 2, NC)),
            dma, dma((LAYERS,)), dma((4,)), dma((2,)),
        ]
        out, loss = pl.pallas_call(
            kernel,
            out_shape=(jax.ShapeDtypeStruct((dim, shard + nitem // 2), BF16),
                       jax.ShapeDtypeStruct((8, 128), F32)),
            in_specs=[hbm, hbm, hbm, hbm],
            out_specs=(hbm, vmem),
            scratch_shapes=scratch,
            compiler_params=pltpu.CompilerParams(collective_id=0, has_side_effects=True,
                                                 vmem_limit_bytes=67043328),
        )(mask_blk, user_shard.T, item_shard.T, triples.T)
        out_user, out_item, loss = pl.pallas_call(
            split_kernel,
            out_shape=(jax.ShapeDtypeStruct((dim, shard), BF16), jax.ShapeDtypeStruct((dim, nitem // 2), BF16),
                       jax.ShapeDtypeStruct((1, 1), F32)),
            in_specs=[hbm, hbm],
            out_specs=(hbm, hbm, hbm),
            scratch_shapes=[pltpu.VMEM((dim, shard + nitem // 2), BF16), pltpu.VMEM((8, 128), F32), pltpu.VMEM((1, 1), F32), dma((6,)), dma((6,))],
        )(out, loss)
        return out_user.T, out_item.T, loss[0, 0]

    return jax.shard_map(local_prog, mesh=mesh, in_specs=(P("row", "col"), P(("row", "col"), None), P(("col", "row"), None), P(None, None)),
                         out_specs=(P(("row", "col"), None), P(("col", "row"), None), P()), check_vma=False)
```

```python
import functools

import jax
import jax.numpy as jnp
from jax import lax
from jax.experimental import pallas as pl
from jax.experimental.pallas import tpu as pltpu
from jax.sharding import PartitionSpec as P

LAYERS = 3
NC = 4
MESH = pl.DeviceIdType.MESH
F32 = jnp.float32
BF16 = jnp.bfloat16
NT = (((1,), (1,)), ((), ()))


def flip(v, f):
    return v + f - 2 * v * f


def kernel(mask, emb_user, emb_item, triples, out, loss,
           adj, ring, part, recv1, recv2, table, acc, racc, items, ei_half, trip,
           rowsum, deg, rdeg, dsum, col, rcol, su, sv, ubuf, ibuf, picks, rpicks, rows, tsum, hots, lbuf,
           ring_sem, in_sem, item_sem, deg_s, deg_r, col_sem, ag0_s, ag0_r, sent, r1, r2, ag_s, ag_r, acc_s, acc_r,
           pick_sem, loss_sem):
    users, nitem = mask.shape
    shard = users // 4
    half = shard // 2
    width = half // NC
    nhalf = nitem // 2
    ntrip = triples.shape[1]
    c = lax.axis_index("col")
    r = lax.axis_index("row")
    x = c % 2
    y = c // 2
    nx = y * 2 + 1 - x
    ny = (1 - y) * 2 + x
    nd = (1 - y) * 2 + 1 - x

    def dev(col_id):
        return {"col": col_id, "row": r}

    partner = {"col": c, "row": 1 - r}

    def remote(src, dst, ss, rs, device):
        return pltpu.make_async_remote_copy(src_ref=src, dst_ref=dst, send_sem=ss, recv_sem=rs,
                                            device_id=device, device_id_type=MESH)

    def wait_bytes(ref, sem):
        pltpu.make_async_copy(ref, ref, sem).wait()

    blk = ring.shape[1]
    nslot = ring.shape[0]
    nblk = users // blk

    def mask_row(b):
        q = b * blk // width
        return (q % 8 // 2) * shard + (q % 2) * half + (q // 8) * width + (b * blk) % width

    def mask_copy(b, slot):
        rows = pl.ds(pl.multiple_of(mask_row(b), blk), blk)
        return pltpu.make_async_copy(mask.at[rows], ring.at[slot], ring_sem.at[slot])

    for b in range(nslot):
        mask_copy(b, b).start()

    def user_cols(hh, k):
        return emb_user.at[:, pl.ds(hh * half + k * width, width)]

    def user_in(hh, k):
        return pltpu.make_async_copy(user_cols(hh, k), table.at[0, 0, hh, k], in_sem.at[0])

    for hh in range(2):
        for k in range(NC):
            user_in(hh, k).start()
    ci = pltpu.make_async_copy(emb_item, ei_half.at[r], in_sem.at[1])
    ct = pltpu.make_async_copy(triples, trip, in_sem.at[2])
    ci.start()
    ct.start()

    barrier = pltpu.get_barrier_semaphore()
    for dc in (c, nx, ny, nd):
        for dr in (r, 1 - r):
            if dc is c and dr is r:
                continue
            pl.semaphore_signal(barrier, inc=1, device_id={"col": dc, "row": dr}, device_id_type=MESH)

    ic = remote(ei_half.at[r], ei_half.at[r], item_sem.at[0], item_sem.at[1], partner)

    def ag0_start(d, hh):
        for k in range(NC):
            remote(user_cols(hh, k), table.at[0, 1 + d, hh, k], ag0_s, ag0_r.at[hh if d == hh else 2],
                   dev(nx if d == 0 else ny)).start()

    def fw0(hh, part_id):
        ks = pl.ds(part_id * (NC // 2), NC // 2)
        return remote(table.at[0, 1 + hh, hh, ks], table.at[0, 3, hh, ks], ag0_s, ag0_r.at[2 + part_id],
                      dev(ny if hh == 0 else nx))

    def share_tables():
        pl.semaphore_wait(barrier, 7)
        for hh in range(2):
            ag0_start(hh, hh)

    strip = 64
    col[...] = jnp.zeros_like(col)
    ones = jnp.ones((16, 128), BF16)
    sub8 = lax.broadcasted_iota(jnp.int32, (8, 128), 0)
    pair = 2 * width
    nsub = pair // blk
    groups = pair // 128

    def read_pair(i):
        turn = i % (nslot // nsub)
        for u in range(nsub):
            b = i * nsub + u
            slot = turn * nsub + u
            arow = mask_row(b)
            mask_copy(b, slot).wait()

            def strips(q, colacc):
                r0 = pl.multiple_of(q * strip, strip)
                m = ring[slot, pl.ds(r0, strip), :]
                mb = m.astype(F32).astype(BF16)
                adj[pl.ds(pl.multiple_of(arow + q * strip, strip), strip), :] = mb
                rsum = mb[:, 0:128]
                for j in range(1, nitem // 128):
                    rsum = rsum + mb[:, j * 128:(j + 1) * 128]
                rowsum[pl.ds(pl.multiple_of(u * blk + q * strip, strip), strip), :] = rsum
                for j in range(strip // 8):
                    colacc = colacc + m[j * 8:(j + 1) * 8, :]
                return colacc

            colacc = lax.fori_loop(0, blk // strip, strips, jnp.zeros((8, nitem), jnp.int32), unroll=2)
            col[...] += colacc.astype(F32)

            @pl.when(b + nslot < nblk)
            def _():
                mask_copy(b + nslot, slot).start()

        rd = lax.dot_general(ones, rowsum[...], NT, preferred_element_type=F32)[0:8]
        comp = jnp.zeros((8, 128), F32)
        for j in range(groups):
            comp = jnp.where(sub8 == j, rd[:, j * 128:(j + 1) * 128], comp)
        deg[pl.ds(pl.multiple_of(i * groups, groups), groups), :] = comp

    npair = users // pair
    per = npair // 4
    drows = deg.shape[0] // 4

    def deg_rows(p):
        return pl.ds(p * drows, drows)

    def deg_x(p):
        return remote(deg.at[deg_rows(p)], rdeg.at[0, deg_rows(p)], deg_s, deg_r.at[0, p], dev(nx))

    def deg_y(p):
        return remote(dsum.at[deg_rows(p)], rdeg.at[1, deg_rows(p)], deg_s, deg_r.at[1, p], dev(ny))

    def deg_turn(p):
        deg_x(p).wait_recv()
        dsum[deg_rows(p)] = deg[deg_rows(p)] + rdeg[0, deg_rows(p)]
        deg_y(p).start()

    for p in range(4):
        def read_body(i, carry):
            read_pair(p * per + i)
            return carry

        if p == 0:
            share_tables()
        cut = per // 2 if p >= 2 else 0
        if cut:
            lax.fori_loop(0, cut, read_body, 0)
            deg_turn(p - 2)
        if p == 2:
            for hh in range(2):
                wait_bytes(table.at[0, 1 + hh, hh], ag0_r.at[hh])
                fw0(hh, 0).start()
        if p == 3:
            for hh in range(2):
                fw0(hh, 1).start()
        lax.fori_loop(cut, per, read_body, 0)
        if p == 3:
            remote(col, rcol, col_sem.at[0], col_sem.at[1], partner).start()
        deg_x(p).start()
        if p == 0:
            for hh in range(2):
                ag0_start(1 - hh, hh)
            ci.wait()
            ct.wait()
            ic.start()
    wait_bytes(table.at[0, 0], in_sem.at[0])
    ic.wait()
    items[0, :, 0:nhalf] = ei_half[0]
    items[0, :, nhalf:] = ei_half[1]
    remote(col, rcol, col_sem.at[0], col_sem.at[1], partner).wait()
    dv = jnp.sum(col[...] + rcol[...], axis=0, keepdims=True)
    sv[...] = jnp.broadcast_to(lax.rsqrt(jnp.maximum(dv, 1.0)), sv.shape)

    def row_of(shard_id, hh, k):
        return pl.multiple_of(shard_id * shard + hh * half + k * width, width)

    def user_scale(k):
        sl = deg_rows(k)
        deg_y(k).wait_recv()
        su[sl] = lax.rsqrt(jnp.maximum(dsum[sl] + rdeg[1, sl], 1.0))

    def build(row0, g0, count):
        for g in range(count):
            sc = jnp.broadcast_to(su[pl.ds(g0 + g, 1), :], (128, 128)).T
            rows = pl.ds(pl.multiple_of(row0 + g * 128, 128), 128)
            for j in range(nitem // 128):
                cols = slice(j * 128, (j + 1) * 128)
                adj[rows, cols] = adj[rows, cols] * (sc * sv[0:1, cols]).astype(BF16)

    def send1(hh, k, t):
        nb = (1 - hh) * nx + hh * ny
        return remote(part.at[hh, k, t], recv1.at[hh, k, t], sent.at[k], r1.at[hh, k, t], dev(nb))

    def send2(hh, k):
        nb = (1 - hh) * ny + hh * nx
        return remote(part.at[hh, k, 2], recv2.at[hh, k], sent.at[k], r2.at[hh, k], dev(nb))

    def ag(j, d, hh, k):
        return remote(table.at[j, 0, hh, k], table.at[j, 1 + d, hh, k], ag_s.at[j - 1],
                      ag_r.at[j - 1, 0 if d == hh else 1, k],
                      dev(nx if d == 0 else ny))

    def fw(j, hh, k):
        return remote(table.at[j, 1 + hh, hh, k], table.at[j, 3, hh, k], ag_s.at[j - 1], ag_r.at[j - 1, 1, k],
                      dev(ny if hh == 0 else nx))

    def sends_done(k):
        wait_bytes(part.at[0, pl.ds(0, 3), pl.ds(0, 2)], sent.at[k])

    def product(j, k, lo=0, hi=8):
        if j > 0:
            sends_done(k)
        elif lo == 0:
            if k < 2:
                deg_turn(2 + k)
            user_scale(k)

        piece = width // 2

        def lead(i, carry):
            q = i // 2
            hh = i % 2
            owner = 3 - c
            row0 = row_of(owner, hh, k) + q * piece
            build(row0, ((k * 4 + owner) * 2 + hh) * (width // 128) + q * (piece // 128), piece // 128)
            cols = pl.ds(pl.multiple_of(q * piece, piece), piece)
            part[hh, k, 0, :, cols] = lax.dot_general(items[j], adj[pl.ds(pl.multiple_of(row0, piece), piece), :], NT,
                                                      preferred_element_type=F32)
            nb = (1 - hh) * nx + hh * ny
            remote(part.at[hh, k, 0, :, cols], recv1.at[hh, k, 0, :, cols], sent.at[k], r1.at[hh, k, 0], dev(nb)).start()
            return carry

        if j == 0 and k == 0 and lo == 0:
            lax.fori_loop(0, 2 * (width // piece), lead, 0)
            lo = 2

        def body(i, carry):
            t = i // 2
            hh = i % 2
            fa = 1 - t // 2
            fb = 1 - t % 2
            fx = fa * (1 - hh) + fb * hh
            fy = fb * (1 - hh) + fa * hh
            owner = flip(y, fy) * 2 + flip(x, fx)
            row0 = row_of(owner, hh, k)
            if j == 0:
                build(row0, ((k * 4 + owner) * 2 + hh) * (width // 128), width // 128)
            part[hh, k, t] = lax.dot_general(items[j], adj[pl.ds(row0, width), :], NT, preferred_element_type=F32)

            @pl.when(t < 2)
            def _():
                send1(hh, k, t).start()

            return carry

        lax.fori_loop(lo, hi, body, 0)

    def step2(k):
        for hh in range(2):
            send1(hh, k, 0).wait_recv()
            part[hh, k, 2] = part[hh, k, 2] + recv1[hh, k, 0]
            send2(hh, k).start()

    def last(j, k):
        if j + 1 < LAYERS:
            for hh in range(2):
                send1(hh, k, 1).wait_recv()
                send2(hh, k).wait_recv()
                table[j + 1, 0, hh, k] = (part[hh, k, 3] + recv1[hh, k, 1] + recv2[hh, k]).astype(BF16)
                ag(j + 1, hh, hh, k).start()
                ag(j + 1, 1 - hh, hh, k).start()
            return
        for hh in range(2):
            send1(hh, k, 1).wait_recv()
            part[hh, k, 3] = part[hh, k, 3] + recv1[hh, k, 1]
            tot = table[0, 0, hh, k].astype(F32) + table[1, 0, hh, k].astype(F32)
            tsum[hh] = tot + table[2, 0, hh, k].astype(F32)
            base = (r * 4 + c) * shard + hh * half + k * width
            ids = lax.broadcasted_iota(jnp.int32, (width, ntrip), 0) + base
            hots[hh] = jnp.where(trip[0:1, :] == ids, 1.0, 0.0).astype(BF16)
        for hh in range(2):
            send2(hh, k).wait_recv()
            res = (part[hh, k, 3] + recv2[hh, k]).astype(BF16)
            o = ((tsum[hh] + res.astype(F32)) * (1.0 / (LAYERS + 1))).astype(BF16)
            ubuf[hh, k] = o
            ucopy(hh, k).start()
            picks[...] += jnp.dot(o, hots[hh], preferred_element_type=F32)

    def ucopy(hh, k):
        cols = pl.ds(hh * half + k * width, width)
        return pltpu.make_async_copy(ubuf.at[hh, k], out.at[:, cols], in_sem.at[0])

    def forward(j, k):
        wait_bytes(table.at[j + 1, pl.ds(0, 2), 0, k], ag_r.at[j, 0, k])
        for hh in range(2):
            fw(j + 1, hh, k).start()

    def gather_item(j, k):
        if j == 0:
            if k == 0:
                wait_bytes(table.at[0, pl.ds(0, 3), 0], ag0_r.at[2])
            if k == NC // 2:
                wait_bytes(table.at[0, 3, 0], ag0_r.at[3])
        else:
            wait_bytes(table.at[j, pl.ds(0, 4), 0, k], ag_r.at[j - 1, 1, k])

        def body(i, carry):
            q = i // 2
            hh = i % 2
            row0 = row_of(flip(y, q // 2) * 2 + flip(x, q % 2), hh, k)
            acc[...] += jnp.dot(table[j, q, hh, k], adj[pl.ds(row0, width), :], preferred_element_type=F32)
            return carry

        lax.fori_loop(0, 8, body, 0)

    def acc_copy(j):
        return remote(acc, racc.at[j], acc_s, acc_r.at[j], partner)

    def item_next(j):
        acc_copy(j).wait()
        items[j + 1] = (acc[...] + racc[j]).astype(BF16)
        if j + 1 < LAYERS:
            acc[...] = jnp.zeros_like(acc)

    def pick_copy(d):
        return remote(rpicks.at[0], rpicks.at[1 + d], pick_sem.at[0], pick_sem.at[1], dev((nx, ny, nd)[d]))

    def rows_copy():
        return remote(rows.at[r], rows.at[r], pick_sem.at[2], pick_sem.at[3], partner)

    def pick_swap():
        wait_bytes(rpicks.at[pl.ds(1, 3)], pick_sem.at[1])
        row = rpicks[0].astype(F32)
        for d in range(3):
            row = row + rpicks[1 + d].astype(F32)
        rows[r] = row.astype(BF16)
        rows_copy().start()

    def finish_items():
        item_next(LAYERS - 1)
        tot = items[0].astype(F32) + items[1].astype(F32)
        tot = (tot + items[2].astype(F32)) + items[3].astype(F32)
        o = (tot * (1.0 / (LAYERS + 1))).astype(BF16)
        ibuf[0] = o[:, 0:nhalf]
        ibuf[1] = o[:, nhalf:]
        pltpu.make_async_copy(ibuf.at[r], out.at[:, pl.ds(shard, nhalf)], in_sem.at[1]).start()
        ids = lax.broadcasted_iota(jnp.int32, (nitem, ntrip), 0) + c * nitem
        hot = jnp.where(trip[pl.ds(1 + r, 1), :] == ids, 1.0, 0.0).astype(BF16)
        rpicks[0] = jnp.dot(o, hot, preferred_element_type=F32).astype(BF16)
        for d in range(3):
            pick_copy(d).start()

    acc[...] = jnp.zeros_like(acc)
    picks[...] = jnp.zeros_like(picks)

    total = LAYERS * NC
    def sent_part(k):
        product(0, k, 0, 4)

    def kept_part(k):
        product(0, k, 4, 8)

    sent_part(0)
    sent_part(1)
    kept_part(0)
    step2(0)
    kept_part(1)
    sent_part(2)
    step2(1)
    kept_part(2)
    last(0, 0)
    sent_part(3)
    step2(2)
    kept_part(3)
    last(0, 1)
    gather_item(0, 0)
    forward(0, 0)
    gather_item(0, 1)
    gather_item(0, 2)
    step2(3)
    gather_item(0, 3)
    acc_copy(0).start()
    last(0, 2)
    item_next(0)
    product(1, 0)
    forward(0, 1)
    gather_item(1, 0)

    for g in range(NC + 1, total + 2):
        j, k = g // NC, g % NC
        edge = k == 0
        if g < total and not edge:
            product(j, k)
        if g == total:
            finish_items()
        if g - 1 < total:
            step2((g - 1) % NC)
        if g == total - 1:
            gather_item(j, k)
            acc_copy(j).start()
        last((g - 2) // NC, (g - 2) % NC)
        if g == total:
            pick_swap()
        if (g - 3) // NC + 1 < LAYERS:
            forward((g - 3) // NC, (g - 3) % NC)
        if g < total and edge:
            item_next(j - 1)
            product(j, k)
        if g < total - 1:
            gather_item(j, k)
            if k == NC - 1:
                acc_copy(j).start()

    rows_copy().wait()
    row_p = rows[0].astype(F32)
    row_n = rows[1].astype(F32)
    margin = (jnp.sum(picks[...] * row_p, axis=0, keepdims=True)
              - jnp.sum(picks[...] * row_n, axis=0, keepdims=True))
    neg = -margin
    soft = jnp.maximum(neg, 0.0) + jnp.log1p(jnp.exp(-jnp.abs(neg)))
    me = r * 4 + c
    lid = trip[0:1, :] - me * shard
    soft = jnp.where((lid >= 0) & (lid < shard), soft, 0.0)
    lbuf[me] = jnp.broadcast_to(jnp.sum(soft, axis=1, keepdims=True), (8, 128))

    def loss_copy(n, dc, dr):
        return remote(lbuf.at[me], lbuf.at[me], loss_sem.at[0], loss_sem.at[1], {"col": dc, "row": dr})

    others = [(nx, r), (ny, r), (nd, r), (c, 1 - r), (nx, 1 - r), (ny, 1 - r), (nd, 1 - r)]
    for n, (dc, dr) in enumerate(others):
        loss_copy(n, dc, dr).start()
    wait_bytes(lbuf.at[pl.ds(0, 7)], loss_sem.at[1])
    tot = lbuf[0]
    for n in range(1, 8):
        tot = tot + lbuf[n]
    loss[...] = tot * (1.0 / ntrip)

    wait_bytes(ubuf, in_sem.at[0])
    for k in range(NC):
        sends_done(k)
    for j in range(1, LAYERS):
        wait_bytes(table.at[j, pl.ds(0, 3)], ag_s.at[j - 1])
    wait_bytes(table.at[0, pl.ds(0, 3)], ag0_s)
    wait_bytes(rdeg, deg_s)
    wait_bytes(rpicks.at[pl.ds(1, 3)], pick_sem.at[0])
    wait_bytes(lbuf.at[pl.ds(0, 7)], loss_sem.at[0])
    pltpu.make_async_copy(ibuf.at[r], out.at[:, pl.ds(shard, nhalf)], in_sem.at[1]).wait()


def split_kernel(both, one, out_user, out_item, out_one, buf, one_buf, one_val, in_sem, out_sem):
    shard = out_user.shape[1]
    step = shard // 4
    spans = [(n * step, step) for n in range(4)] + [(shard, out_item.shape[1])]
    loads = [pltpu.make_async_copy(both.at[:, pl.ds(o, w)], buf.at[:, pl.ds(o, w)], in_sem.at[n])
             for n, (o, w) in enumerate(spans)]
    stores = [pltpu.make_async_copy(buf.at[:, pl.ds(o, w)],
                                    out_user.at[:, pl.ds(o, w)] if o < shard else out_item, out_sem.at[n])
              for n, (o, w) in enumerate(spans)]
    loads.insert(0, pltpu.make_async_copy(one, one_buf, in_sem.at[5]))
    stores.insert(0, pltpu.make_async_copy(one_val, out_one, out_sem.at[5]))
    for cp in loads:
        cp.start()
    for n, (ld, st) in enumerate(zip(loads, stores)):
        ld.wait()
        if n == 0:
            one_val[...] = one_buf[0:1, 0:1]
        st.start()
    for st in stores:
        st.wait()


def solution(mesh):
    def local_prog(mask_blk, user_shard, item_shard, triples):
        users, nitem = mask_blk.shape
        shard, dim = user_shard.shape
        trip = triples.shape[0]
        width = shard // 2 // NC
        hbm = pl.BlockSpec(memory_space=pl.ANY)
        vmem = pl.BlockSpec(memory_space=pltpu.VMEM)
        dma = pltpu.SemaphoreType.DMA
        scratch = [
            pltpu.VMEM((users, nitem), BF16),
            pltpu.VMEM((12, 256, nitem), jnp.int32),
            pltpu.VMEM((2, NC, 4, dim, width), F32),
            pltpu.VMEM((2, NC, 2, dim, width), F32),
            pltpu.VMEM((2, NC, dim, width), F32),
            pltpu.VMEM((LAYERS, 4, 2, NC, dim, width), BF16),
            pltpu.VMEM((dim, nitem), F32),
            pltpu.VMEM((LAYERS, dim, nitem), F32),
            pltpu.VMEM((LAYERS + 1, dim, nitem), BF16),
            pltpu.VMEM((2, dim, nitem // 2), BF16),
            pltpu.VMEM((3, trip), jnp.int32),
            pltpu.VMEM((2 * width, 128), BF16),
            pltpu.VMEM((users // 128, 128), F32),
            pltpu.VMEM((2, users // 128, 128), F32),
            pltpu.VMEM((users // 128, 128), F32),
            pltpu.VMEM((8, nitem), F32),
            pltpu.VMEM((8, nitem), F32),
            pltpu.VMEM((users // 128, 128), F32),
            pltpu.VMEM((8, nitem), F32),
            pltpu.VMEM((2, NC, dim, width), BF16),
            pltpu.VMEM((2, dim, nitem // 2), BF16),
            pltpu.VMEM((dim, trip), F32),
            pltpu.VMEM((4, dim, trip), BF16),
            pltpu.VMEM((2, dim, trip), BF16),
            pltpu.VMEM((2, dim, width), F32),
            pltpu.VMEM((2, width, trip), BF16),
            pltpu.VMEM((8, 8, 128), F32),
            dma((12,)), dma((3,)), dma((2,)), dma, dma((2, 4)), dma((2,)),
            dma, dma((4,)),
            dma((NC,)), dma((2, NC, 2)), dma((2, NC)),
            dma((LAYERS - 1,)), dma((LAYERS - 1, 2, NC)),
            dma, dma((LAYERS,)), dma((4,)), dma((2,)),
        ]
        out, loss = pl.pallas_call(
            kernel,
            out_shape=(jax.ShapeDtypeStruct((dim, shard + nitem // 2), BF16),
                       jax.ShapeDtypeStruct((8, 128), F32)),
            in_specs=[hbm, hbm, hbm, hbm],
            out_specs=(hbm, vmem),
            scratch_shapes=scratch,
            compiler_params=pltpu.CompilerParams(collective_id=0, has_side_effects=True,
                                                 vmem_limit_bytes=67043328),
        )(mask_blk, user_shard.T, item_shard.T, triples.T)
        out_user, out_item, loss = pl.pallas_call(
            split_kernel,
            out_shape=(jax.ShapeDtypeStruct((dim, shard), BF16), jax.ShapeDtypeStruct((dim, nitem // 2), BF16),
                       jax.ShapeDtypeStruct((1, 1), F32)),
            in_specs=[hbm, hbm],
            out_specs=(hbm, hbm, hbm),
            scratch_shapes=[pltpu.VMEM((dim, shard + nitem // 2), BF16), pltpu.VMEM((8, 128), F32), pltpu.VMEM((1, 1), F32), dma((6,)), dma((6,))],
        )(out, loss)
        return out_user.T, out_item.T, loss[0, 0]

    return jax.shard_map(local_prog, mesh=mesh, in_specs=(P("row", "col"), P(("row", "col"), None), P(("col", "row"), None), P(None, None)),
                         out_specs=(P(("row", "col"), None), P(("col", "row"), None), P()), check_vma=False)
```

```python
import functools

import jax
import jax.numpy as jnp
from jax import lax
from jax.experimental import pallas as pl
from jax.experimental.pallas import tpu as pltpu
from jax.sharding import PartitionSpec as P

LAYERS = 3
NC = 4
MESH = pl.DeviceIdType.MESH
F32 = jnp.float32
BF16 = jnp.bfloat16
NT = (((1,), (1,)), ((), ()))


def flip(v, f):
    return v + f - 2 * v * f


def kernel(mask, emb_user, emb_item, triples, out, loss,
           adj, ring, part, recv1, recv2, table, acc, racc, items, ei_half, trip,
           rowsum, deg, rdeg, dsum, col, rcol, su, sv, ubuf, ibuf, picks, rpicks, rows, tsum, hots, lbuf,
           ring_sem, in_sem, item_sem, deg_s, deg_r, col_sem, ag0_s, ag0_r, r1, r2, ag_r, acc_r,
           pick_sem, loss_sem):
    users, nitem = mask.shape
    shard = users // 4
    half = shard // 2
    width = half // NC
    nhalf = nitem // 2
    ntrip = triples.shape[1]
    c = lax.axis_index("col")
    r = lax.axis_index("row")
    x = c % 2
    y = c // 2
    nx = y * 2 + 1 - x
    ny = (1 - y) * 2 + x
    nd = (1 - y) * 2 + 1 - x

    def dev(col_id):
        return {"col": col_id, "row": r}

    partner = {"col": c, "row": 1 - r}

    def remote(src, dst, ss, rs, device):
        return pltpu.make_async_remote_copy(src_ref=src, dst_ref=dst, send_sem=ss, recv_sem=rs,
                                            device_id=device, device_id_type=MESH)

    def wait_bytes(ref, sem):
        pltpu.make_async_copy(ref, ref, sem).wait()

    blk = ring.shape[1]
    nslot = ring.shape[0]
    nblk = users // blk

    def mask_row(b):
        q = b * blk // width
        return (q % 8 // 2) * shard + (q % 2) * half + (q // 8) * width + (b * blk) % width

    def mask_copy(b, slot):
        rows = pl.ds(pl.multiple_of(mask_row(b), blk), blk)
        return pltpu.make_async_copy(mask.at[rows], ring.at[slot], ring_sem.at[slot])

    for b in range(nslot):
        mask_copy(b, b).start()

    def user_cols(hh, k):
        return emb_user.at[:, pl.ds(hh * half + k * width, width)]

    def user_in(hh, k):
        return pltpu.make_async_copy(user_cols(hh, k), table.at[0, 0, hh, k], in_sem.at[0])

    for hh in range(2):
        for k in range(NC):
            user_in(hh, k).start()
    ci = pltpu.make_async_copy(emb_item, ei_half.at[r], in_sem.at[1])
    ct = pltpu.make_async_copy(triples, trip, in_sem.at[2])
    ci.start()
    ct.start()

    barrier = pltpu.get_barrier_semaphore()
    for dc in (c, nx, ny, nd):
        for dr in (r, 1 - r):
            if dc is c and dr is r:
                continue
            pl.semaphore_signal(barrier, inc=1, device_id={"col": dc, "row": dr}, device_id_type=MESH)

    ic = remote(ei_half.at[r], ei_half.at[r], item_sem.at[0], item_sem.at[1], partner)

    def ag0_start(d, hh):
        for k in range(NC):
            remote(user_cols(hh, k), table.at[0, 1 + d, hh, k], ag0_s, ag0_r.at[hh if d == hh else 2],
                   dev(nx if d == 0 else ny)).start()

    def fw0(hh, part_id):
        ks = pl.ds(part_id * (NC // 2), NC // 2)
        return remote(table.at[0, 1 + hh, hh, ks], table.at[0, 3, hh, ks], ag0_s, ag0_r.at[2 + part_id],
                      dev(ny if hh == 0 else nx))

    def share_tables():
        pl.semaphore_wait(barrier, 7)
        for hh in range(2):
            ag0_start(hh, hh)

    strip = 64
    col[...] = jnp.zeros_like(col)
    ones = jnp.ones((16, 128), BF16)
    sub8 = lax.broadcasted_iota(jnp.int32, (8, 128), 0)
    pair = 2 * width
    nsub = pair // blk
    groups = pair // 128

    def read_pair(i):
        turn = i % (nslot // nsub)
        for u in range(nsub):
            b = i * nsub + u
            slot = turn * nsub + u
            arow = mask_row(b)
            mask_copy(b, slot).wait()

            def strips(q, colacc):
                r0 = pl.multiple_of(q * strip, strip)
                m = ring[slot, pl.ds(r0, strip), :]
                mb = m.astype(F32).astype(BF16)
                adj[pl.ds(pl.multiple_of(arow + q * strip, strip), strip), :] = mb
                rsum = mb[:, 0:128]
                for j in range(1, nitem // 128):
                    rsum = rsum + mb[:, j * 128:(j + 1) * 128]
                rowsum[pl.ds(pl.multiple_of(u * blk + q * strip, strip), strip), :] = rsum
                for j in range(strip // 8):
                    colacc = colacc + m[j * 8:(j + 1) * 8, :]
                return colacc

            colacc = lax.fori_loop(0, blk // strip, strips, jnp.zeros((8, nitem), jnp.int32), unroll=2)
            col[...] += colacc.astype(F32)

            @pl.when(b + nslot < nblk)
            def _():
                mask_copy(b + nslot, slot).start()

        rd = lax.dot_general(ones, rowsum[...], NT, preferred_element_type=F32)[0:8]
        comp = jnp.zeros((8, 128), F32)
        for j in range(groups):
            comp = jnp.where(sub8 == j, rd[:, j * 128:(j + 1) * 128], comp)
        deg[pl.ds(pl.multiple_of(i * groups, groups), groups), :] = comp

    npair = users // pair
    per = npair // 4
    drows = deg.shape[0] // 4

    def deg_rows(p):
        return pl.ds(p * drows, drows)

    def deg_x(p):
        return remote(deg.at[deg_rows(p)], rdeg.at[0, deg_rows(p)], deg_s, deg_r.at[0, p], dev(nx))

    def deg_y(p):
        return remote(dsum.at[deg_rows(p)], rdeg.at[1, deg_rows(p)], deg_s, deg_r.at[1, p], dev(ny))

    def deg_turn(p):
        deg_x(p).wait_recv()
        dsum[deg_rows(p)] = deg[deg_rows(p)] + rdeg[0, deg_rows(p)]
        deg_y(p).start()

    for p in range(4):
        def read_body(i, carry):
            read_pair(p * per + i)
            return carry

        if p == 0:
            share_tables()
        cut = per // 2 if p >= 2 else 0
        if cut:
            lax.fori_loop(0, cut, read_body, 0)
            deg_turn(p - 2)
        if p == 2:
            for hh in range(2):
                wait_bytes(table.at[0, 1 + hh, hh], ag0_r.at[hh])
                fw0(hh, 0).start()
        if p == 3:
            for hh in range(2):
                fw0(hh, 1).start()
        lax.fori_loop(cut, per, read_body, 0)
        if p == 3:
            remote(col, rcol, col_sem.at[0], col_sem.at[1], partner).start()
        deg_x(p).start()
        if p == 0:
            for hh in range(2):
                ag0_start(1 - hh, hh)
            ci.wait()
            ct.wait()
            ic.start()
    wait_bytes(table.at[0, 0], in_sem.at[0])
    ic.wait()
    items[0, :, 0:nhalf] = ei_half[0]
    items[0, :, nhalf:] = ei_half[1]
    remote(col, rcol, col_sem.at[0], col_sem.at[1], partner).wait()
    dv = jnp.sum(col[...] + rcol[...], axis=0, keepdims=True)
    sv[...] = jnp.broadcast_to(lax.rsqrt(jnp.maximum(dv, 1.0)), sv.shape)

    def row_of(shard_id, hh, k):
        return pl.multiple_of(shard_id * shard + hh * half + k * width, width)

    def user_scale(k):
        sl = deg_rows(k)
        deg_y(k).wait_recv()
        su[sl] = lax.rsqrt(jnp.maximum(dsum[sl] + rdeg[1, sl], 1.0))

    def build(row0, g0, count):
        for g in range(count):
            sc = jnp.broadcast_to(su[pl.ds(g0 + g, 1), :], (128, 128)).T
            rows = pl.ds(pl.multiple_of(row0 + g * 128, 128), 128)
            for j in range(nitem // 128):
                cols = slice(j * 128, (j + 1) * 128)
                adj[rows, cols] = adj[rows, cols] * (sc * sv[0:1, cols]).astype(BF16)

    def send1(hh, k, t):
        nb = (1 - hh) * nx + hh * ny
        return remote(part.at[hh, k, t], recv1.at[hh, k, t], ring_sem.at[k], r1.at[hh, k, t], dev(nb))

    def send2(hh, k):
        nb = (1 - hh) * ny + hh * nx
        return remote(part.at[hh, k, 2], recv2.at[hh, k], ring_sem.at[k], r2.at[hh, k], dev(nb))

    def ag(j, d, hh, k):
        return remote(table.at[j, 0, hh, k], table.at[j, 1 + d, hh, k], ring_sem.at[NC + j - 1],
                      ag_r.at[j - 1, 0 if d == hh else 1, k],
                      dev(nx if d == 0 else ny))

    def fw(j, hh, k):
        return remote(table.at[j, 1 + hh, hh, k], table.at[j, 3, hh, k], ring_sem.at[NC + j - 1], ag_r.at[j - 1, 1, k],
                      dev(ny if hh == 0 else nx))

    def sends_done(k):
        wait_bytes(part.at[0, pl.ds(0, 3), pl.ds(0, 2)], ring_sem.at[k])

    def product(j, k, lo=0, hi=8):
        if j > 0:
            sends_done(k)
        elif lo == 0:
            if k < 2:
                deg_turn(2 + k)
            user_scale(k)

        piece = width // 2

        def lead(i, carry):
            q = i // 2
            hh = i % 2
            owner = 3 - c
            row0 = row_of(owner, hh, k) + q * piece
            build(row0, ((k * 4 + owner) * 2 + hh) * (width // 128) + q * (piece // 128), piece // 128)
            cols = pl.ds(pl.multiple_of(q * piece, piece), piece)
            part[hh, k, 0, :, cols] = lax.dot_general(items[j], adj[pl.ds(pl.multiple_of(row0, piece), piece), :], NT,
                                                      preferred_element_type=F32)
            nb = (1 - hh) * nx + hh * ny
            remote(part.at[hh, k, 0, :, cols], recv1.at[hh, k, 0, :, cols], ring_sem.at[k], r1.at[hh, k, 0], dev(nb)).start()
            return carry

        if j == 0 and k == 0 and lo == 0:
            lax.fori_loop(0, 2 * (width // piece), lead, 0)
            lo = 2

        def body(i, carry):
            t = i // 2
            hh = i % 2
            fa = 1 - t // 2
            fb = 1 - t % 2
            fx = fa * (1 - hh) + fb * hh
            fy = fb * (1 - hh) + fa * hh
            owner = flip(y, fy) * 2 + flip(x, fx)
            row0 = row_of(owner, hh, k)
            if j == 0:
                build(row0, ((k * 4 + owner) * 2 + hh) * (width // 128), width // 128)
            part[hh, k, t] = lax.dot_general(items[j], adj[pl.ds(row0, width), :], NT, preferred_element_type=F32)

            @pl.when(t < 2)
            def _():
                send1(hh, k, t).start()

            return carry

        lax.fori_loop(lo, hi, body, 0)

    def step2(k):
        for hh in range(2):
            send1(hh, k, 0).wait_recv()
            part[hh, k, 2] = part[hh, k, 2] + recv1[hh, k, 0]
            send2(hh, k).start()

    def last(j, k):
        if j + 1 < LAYERS:
            for hh in range(2):
                send1(hh, k, 1).wait_recv()
                send2(hh, k).wait_recv()
                table[j + 1, 0, hh, k] = (part[hh, k, 3] + recv1[hh, k, 1] + recv2[hh, k]).astype(BF16)
                ag(j + 1, hh, hh, k).start()
                ag(j + 1, 1 - hh, hh, k).start()
            return
        for hh in range(2):
            send1(hh, k, 1).wait_recv()
            part[hh, k, 3] = part[hh, k, 3] + recv1[hh, k, 1]
            tot = table[0, 0, hh, k].astype(F32) + table[1, 0, hh, k].astype(F32)
            tsum[hh] = tot + table[2, 0, hh, k].astype(F32)
            base = (r * 4 + c) * shard + hh * half + k * width
            ids = lax.broadcasted_iota(jnp.int32, (width, ntrip), 0) + base
            hots[hh] = jnp.where(trip[0:1, :] == ids, 1.0, 0.0).astype(BF16)
        for hh in range(2):
            send2(hh, k).wait_recv()
            res = (part[hh, k, 3] + recv2[hh, k]).astype(BF16)
            o = ((tsum[hh] + res.astype(F32)) * (1.0 / (LAYERS + 1))).astype(BF16)
            ubuf[hh, k] = o
            ucopy(hh, k).start()
            picks[...] += jnp.dot(o, hots[hh], preferred_element_type=F32)

    def ucopy(hh, k):
        cols = pl.ds(hh * half + k * width, width)
        return pltpu.make_async_copy(ubuf.at[hh, k], out.at[:, cols], in_sem.at[0])

    def forward(j, k):
        wait_bytes(table.at[j + 1, pl.ds(0, 2), 0, k], ag_r.at[j, 0, k])
        for hh in range(2):
            fw(j + 1, hh, k).start()

    def gather_item(j, k):
        if j == 0:
            if k == 0:
                wait_bytes(table.at[0, pl.ds(0, 3), 0], ag0_r.at[2])
            if k == NC // 2:
                wait_bytes(table.at[0, 3, 0], ag0_r.at[3])
        else:
            wait_bytes(table.at[j, pl.ds(0, 4), 0, k], ag_r.at[j - 1, 1, k])

        def body(i, carry):
            q = i // 2
            hh = i % 2
            row0 = row_of(flip(y, q // 2) * 2 + flip(x, q % 2), hh, k)
            acc[...] += jnp.dot(table[j, q, hh, k], adj[pl.ds(row0, width), :], preferred_element_type=F32)
            return carry

        lax.fori_loop(0, 8, body, 0)

    def acc_copy(j):
        return remote(acc, racc.at[j], ring_sem.at[NC + 2], acc_r.at[j], partner)

    def item_next(j):
        acc_copy(j).wait()
        items[j + 1] = (acc[...] + racc[j]).astype(BF16)
        if j + 1 < LAYERS:
            acc[...] = jnp.zeros_like(acc)

    def pick_copy(d):
        return remote(rpicks.at[0], rpicks.at[1 + d], ring_sem.at[NC + 3], pick_sem.at[0], dev((nx, ny, nd)[d]))

    def rows_copy():
        return remote(rows.at[r], rows.at[r], ring_sem.at[NC + 4], pick_sem.at[1], partner)

    def pick_swap():
        wait_bytes(rpicks.at[pl.ds(1, 3)], pick_sem.at[0])
        row = rpicks[0].astype(F32)
        for d in range(3):
            row = row + rpicks[1 + d].astype(F32)
        rows[r] = row.astype(BF16)
        rows_copy().start()

    def finish_items():
        item_next(LAYERS - 1)
        tot = items[0].astype(F32) + items[1].astype(F32)
        tot = (tot + items[2].astype(F32)) + items[3].astype(F32)
        o = (tot * (1.0 / (LAYERS + 1))).astype(BF16)
        ibuf[0] = o[:, 0:nhalf]
        ibuf[1] = o[:, nhalf:]
        pltpu.make_async_copy(ibuf.at[r], out.at[:, pl.ds(shard, nhalf)], in_sem.at[1]).start()
        ids = lax.broadcasted_iota(jnp.int32, (nitem, ntrip), 0) + c * nitem
        hot = jnp.where(trip[pl.ds(1 + r, 1), :] == ids, 1.0, 0.0).astype(BF16)
        rpicks[0] = jnp.dot(o, hot, preferred_element_type=F32).astype(BF16)
        for d in range(3):
            pick_copy(d).start()

    acc[...] = jnp.zeros_like(acc)
    picks[...] = jnp.zeros_like(picks)

    total = LAYERS * NC
    def sent_part(k):
        product(0, k, 0, 4)

    def kept_part(k):
        product(0, k, 4, 8)

    sent_part(0)
    sent_part(1)
    kept_part(0)
    step2(0)
    kept_part(1)
    sent_part(2)
    step2(1)
    kept_part(2)
    last(0, 0)
    sent_part(3)
    step2(2)
    kept_part(3)
    last(0, 1)
    gather_item(0, 0)
    forward(0, 0)
    gather_item(0, 1)
    gather_item(0, 2)
    step2(3)
    gather_item(0, 3)
    acc_copy(0).start()
    last(0, 2)
    item_next(0)
    product(1, 0)
    forward(0, 1)
    gather_item(1, 0)

    for g in range(NC + 1, total + 2):
        j, k = g // NC, g % NC
        edge = k == 0
        if g < total and not edge:
            product(j, k)
        if g == total:
            finish_items()
        if g - 1 < total:
            step2((g - 1) % NC)
        if g == total - 1:
            gather_item(j, k)
            acc_copy(j).start()
        last((g - 2) // NC, (g - 2) % NC)
        if g == total:
            pick_swap()
        if (g - 3) // NC + 1 < LAYERS:
            forward((g - 3) // NC, (g - 3) % NC)
        if g < total and edge:
            item_next(j - 1)
            product(j, k)
        if g < total - 1:
            gather_item(j, k)
            if k == NC - 1:
                acc_copy(j).start()

    rows_copy().wait()
    row_p = rows[0].astype(F32)
    row_n = rows[1].astype(F32)
    margin = (jnp.sum(picks[...] * row_p, axis=0, keepdims=True)
              - jnp.sum(picks[...] * row_n, axis=0, keepdims=True))
    neg = -margin
    soft = jnp.maximum(neg, 0.0) + jnp.log1p(jnp.exp(-jnp.abs(neg)))
    me = r * 4 + c
    lid = trip[0:1, :] - me * shard
    soft = jnp.where((lid >= 0) & (lid < shard), soft, 0.0)
    lbuf[me] = jnp.broadcast_to(jnp.sum(soft, axis=1, keepdims=True), (8, 128))

    def loss_copy(n, dc, dr):
        return remote(lbuf.at[me], lbuf.at[me], ring_sem.at[NC + 5], loss_sem, {"col": dc, "row": dr})

    others = [(nx, r), (ny, r), (nd, r), (c, 1 - r), (nx, 1 - r), (ny, 1 - r), (nd, 1 - r)]
    for n, (dc, dr) in enumerate(others):
        loss_copy(n, dc, dr).start()
    wait_bytes(lbuf.at[pl.ds(0, 7)], loss_sem)
    tot = lbuf[0]
    for n in range(1, 8):
        tot = tot + lbuf[n]
    loss[...] = tot * (1.0 / ntrip)

    wait_bytes(ubuf, in_sem.at[0])
    for k in range(NC):
        sends_done(k)
    for j in range(1, LAYERS):
        wait_bytes(table.at[j, pl.ds(0, 3)], ring_sem.at[NC + j - 1])
    wait_bytes(table.at[0, pl.ds(0, 3)], ag0_s)
    wait_bytes(rdeg, deg_s)
    wait_bytes(rpicks.at[pl.ds(1, 3)], ring_sem.at[NC + 3])
    wait_bytes(lbuf.at[pl.ds(0, 7)], ring_sem.at[NC + 5])
    pltpu.make_async_copy(ibuf.at[r], out.at[:, pl.ds(shard, nhalf)], in_sem.at[1]).wait()


def split_kernel(both, one, out_user, out_item, out_one, buf, one_buf, one_val, in_sem, out_sem):
    shard = out_user.shape[1]
    step = shard // 4
    spans = [(n * step, step) for n in range(4)] + [(shard, out_item.shape[1])]
    loads = [pltpu.make_async_copy(both.at[:, pl.ds(o, w)], buf.at[:, pl.ds(o, w)], in_sem.at[n])
             for n, (o, w) in enumerate(spans)]
    stores = [pltpu.make_async_copy(buf.at[:, pl.ds(o, w)],
                                    out_user.at[:, pl.ds(o, w)] if o < shard else out_item, out_sem.at[n])
              for n, (o, w) in enumerate(spans)]
    loads.insert(0, pltpu.make_async_copy(one, one_buf, in_sem.at[5]))
    stores.insert(0, pltpu.make_async_copy(one_val, out_one, out_sem.at[5]))
    for cp in loads:
        cp.start()
    for n, (ld, st) in enumerate(zip(loads, stores)):
        ld.wait()
        if n == 0:
            one_val[...] = one_buf[0:1, 0:1]
        st.start()
    for st in stores:
        st.wait()


def solution(mesh):
    def local_prog(mask_blk, user_shard, item_shard, triples):
        users, nitem = mask_blk.shape
        shard, dim = user_shard.shape
        trip = triples.shape[0]
        width = shard // 2 // NC
        hbm = pl.BlockSpec(memory_space=pl.ANY)
        vmem = pl.BlockSpec(memory_space=pltpu.VMEM)
        dma = pltpu.SemaphoreType.DMA
        scratch = [
            pltpu.VMEM((users, nitem), BF16),
            pltpu.VMEM((12, 256, nitem), jnp.int32),
            pltpu.VMEM((2, NC, 4, dim, width), F32),
            pltpu.VMEM((2, NC, 2, dim, width), F32),
            pltpu.VMEM((2, NC, dim, width), F32),
            pltpu.VMEM((LAYERS, 4, 2, NC, dim, width), BF16),
            pltpu.VMEM((dim, nitem), F32),
            pltpu.VMEM((LAYERS, dim, nitem), F32),
            pltpu.VMEM((LAYERS + 1, dim, nitem), BF16),
            pltpu.VMEM((2, dim, nitem // 2), BF16),
            pltpu.VMEM((3, trip), jnp.int32),
            pltpu.VMEM((2 * width, 128), BF16),
            pltpu.VMEM((users // 128, 128), F32),
            pltpu.VMEM((2, users // 128, 128), F32),
            pltpu.VMEM((users // 128, 128), F32),
            pltpu.VMEM((8, nitem), F32),
            pltpu.VMEM((8, nitem), F32),
            pltpu.VMEM((users // 128, 128), F32),
            pltpu.VMEM((8, nitem), F32),
            pltpu.VMEM((2, NC, dim, width), BF16),
            pltpu.VMEM((2, dim, nitem // 2), BF16),
            pltpu.VMEM((dim, trip), F32),
            pltpu.VMEM((4, dim, trip), BF16),
            pltpu.VMEM((2, dim, trip), BF16),
            pltpu.VMEM((2, dim, width), F32),
            pltpu.VMEM((2, width, trip), BF16),
            pltpu.VMEM((8, 8, 128), F32),
            dma((12,)), dma((3,)), dma((2,)), dma, dma((2, 4)), dma((2,)),
            dma, dma((4,)),
            dma((2, NC, 2)), dma((2, NC)),
            dma((LAYERS - 1, 2, NC)),
            dma((LAYERS,)), dma((2,)), dma,
        ]
        out, loss = pl.pallas_call(
            kernel,
            out_shape=(jax.ShapeDtypeStruct((dim, shard + nitem // 2), BF16),
                       jax.ShapeDtypeStruct((8, 128), F32)),
            in_specs=[hbm, hbm, hbm, hbm],
            out_specs=(hbm, vmem),
            scratch_shapes=scratch,
            compiler_params=pltpu.CompilerParams(collective_id=0, has_side_effects=True,
                                                 vmem_limit_bytes=67043328),
        )(mask_blk, user_shard.T, item_shard.T, triples.T)
        out_user, out_item, loss = pl.pallas_call(
            split_kernel,
            out_shape=(jax.ShapeDtypeStruct((dim, shard), BF16), jax.ShapeDtypeStruct((dim, nitem // 2), BF16),
                       jax.ShapeDtypeStruct((1, 1), F32)),
            in_specs=[hbm, hbm],
            out_specs=(hbm, hbm, hbm),
            scratch_shapes=[pltpu.VMEM((dim, shard + nitem // 2), BF16), pltpu.VMEM((8, 128), F32), pltpu.VMEM((1, 1), F32), dma((6,)), dma((6,))],
        )(out, loss)
        return out_user.T, out_item.T, loss[0, 0]

    return jax.shard_map(local_prog, mesh=mesh, in_specs=(P("row", "col"), P(("row", "col"), None), P(("col", "row"), None), P(None, None)),
                         out_specs=(P(("row", "col"), None), P(("col", "row"), None), P()), check_vma=False)
```
